32 devices in a mesh: gx: 4 (over y, x), gy: 2 (over core), gz: 4 (over z).
Axes of the slice: x: 2, y: 2, z: 4, core: 2. Of those that a mesh axis runs over, the one named last changes fastest.
Arguments:
- flow_state: float32 [5, 128, 32, 512], P(None, 'gz', 'gy', 'gx'), may hold values from -5 to 120, as said below
- advection: float32 [3, 5], replicated, may hold values from -400 to 400, as said below
- inverse_x: float32 [5, 128, 128], replicated, may hold values from -1 to 1, as said below
- inverse_y: float32 [5, 16, 16], replicated, may hold values from -1 to 1, as said below
- inverse_z: float32 [5, 32, 32], replicated, may hold values from -1 to 1, as said below
- reduced_x: float32 [5, 16, 16], replicated, as said below
- reduced_y: float32 [5, 8, 8], replicated, as said below
- reduced_z: float32 [5, 16, 16], replicated, as said below
Outputs:
- update: float32 [5, 128, 32, 512], P(None, 'gz', 'gy', 'gx')
- rms_norm: float32 [5], replicated
The draws below stay inside these ranges and needn't reach their ends.
Inputs may be any that keep to these rules, and one draw needn't show every extreme that they name: flow_state[0] (density) lies between 0.5 and 2, and flow_state[4] / density minus half the squared velocity is at least 0.6 in every cell. `advection`: every entry has magnitude between 100 and 400. inverse_x[v] is the inverse of the 128 x 128 matrix with 4 on the diagonal, advection[0, v] / 2 - 2 just above it, -advection[0, v] / 2 - 2 just below it and 0.5 two places off it. inverse_y[v] is the inverse of the 16 x 16 matrix built likewise from advection[1, v]. inverse_z[v] is the inverse of the 32 x 32 matrix built likewise from advection[2, v]. reduced_x[v] is the inverse of I + K, K being the boundary rows and columns of the block inverses times the coupling between blocks, so that S_x equals the exact solution of the banded system along whole x lines with nothing beyond the grid's ends. reduced_y[v] is built likewise for y lines. reduced_z[v] is built likewise for z lines.
All inputs are finite; a program needn't handle non-finite values.
Results may differ from the reference program's by a relative error of at most 0.0002.
Values sent between devices are 32-bit elements.
A program may use at most 64 MiB of HBM per device.

```python
import jax
import jax.numpy as jnp
import numpy as np
from jax import lax

VARS = 5
CX = 128
CY = 16
CZ = 32
NX = 512
NY = 32
NZ = 128


fourth_coef = 0.5


def advection_table(key):
    subkeys = jax.random.split(jax.random.fold_in(key, 17), 2)
    magnitude = 100.0 * 4.0 ** jax.random.uniform(subkeys[0], (3, VARS), jnp.float32)
    signs = 2.0 * jax.random.randint(subkeys[1], (3, VARS), 0, 2).astype(jnp.float32) - 1.0
    return signs * magnitude


def band_matrix(length, speed):
    identity = jnp.eye(length, dtype=jnp.float32)
    upper_band = jnp.eye(length, k=1, dtype=jnp.float32)
    lower_band = jnp.eye(length, k=-1, dtype=jnp.float32)
    second_band = jnp.eye(length, k=2, dtype=jnp.float32) + jnp.eye(length, k=-2, dtype=jnp.float32)
    return (1.0 + 6.0 * fourth_coef) * identity + (0.5 * speed - 4.0 * fourth_coef) * upper_band + (-0.5 * speed - 4.0 * fourth_coef) * lower_band + fourth_coef * second_band


def block_inverse(key, direction, block_len):
    speeds = advection_table(key)[direction]
    return jax.vmap(lambda speed: jnp.linalg.inv(band_matrix(block_len, speed)))(speeds)


def reduced_inverse(key, direction, block_len, blocks):
    speeds = advection_table(key)[direction]
    length = block_len * blocks
    picked = (block_len * np.arange(blocks)[:, None] + np.array([0, 1, block_len - 2, block_len - 1])[None, :]).reshape(-1)

    def single(speed):
        local_block = band_matrix(block_len, speed)
        whole_line = band_matrix(length, speed)
        spread_inv = jnp.kron(jnp.eye(blocks, dtype=jnp.float32), jnp.linalg.inv(local_block))
        coupling = whole_line - jnp.kron(jnp.eye(blocks, dtype=jnp.float32), local_block)
        product = jnp.dot(spread_inv, coupling, precision=lax.Precision.HIGHEST)
        reduced_k = product[picked][:, picked]
        return jnp.linalg.inv(jnp.eye(4 * blocks, dtype=jnp.float32) + reduced_k)
    return jax.vmap(single)(speeds)


def region_envelope(key):
    phases = jax.random.uniform(jax.random.fold_in(key, 29), (2,), jnp.float32, 0.0, 6.2831853)
    along_z = jnp.arange(NZ, dtype=jnp.float32) * (6.2831853 / NZ)
    along_y = jnp.arange(NY, dtype=jnp.float32) * (6.2831853 / NY)
    shape_z = 0.5 + 0.5 * jnp.sin(along_z + phases[0])
    shape_y = 0.5 + 0.5 * jnp.cos(along_y + phases[1])
    envelope = 0.2 + 0.8 * shape_z[:, None] * shape_y[None, :]
    return envelope[:, :, None]


def draw_flow_state(key, part):
    subkeys = jax.random.split(jax.random.fold_in(key, 11), 6)
    grid_shape = (NZ, NY, NX)
    envelope = region_envelope(key)
    density = 0.5 * 4.0 ** jax.random.uniform(subkeys[0], grid_shape, jnp.float32)
    velocity = jnp.clip(0.6 * jax.random.normal(subkeys[1], (3,) + grid_shape, jnp.float32), -2.5, 2.5)
    baseline = jax.random.uniform(subkeys[2], grid_shape, jnp.float32, 0.6, 1.8)
    density = 1.0 + envelope * (density - 1.0)
    velocity = envelope[None] * velocity
    baseline = 0.6 + envelope * (baseline - 0.6)
    cell_total = NZ * NY * NX
    segment = cell_total // 8
    offsets = jax.random.randint(subkeys[3], (8,), 0, segment)
    hot_cells = jnp.arange(8, dtype=jnp.int32) * segment + offsets
    ranking = jax.random.permutation(subkeys[4], 8)
    levels = 10.0 * 1.25 ** ranking.astype(jnp.float32)
    hot_extra = jnp.zeros((cell_total,), jnp.float32).at[hot_cells].add(levels).reshape(grid_shape)
    internal = baseline + hot_extra
    momentum = density * velocity
    energy = density * (internal + 0.5 * jnp.sum(velocity * velocity, axis=0))
    return jnp.stack([density, momentum[0], momentum[1], momentum[2], energy])


def draw_advection(key, part):
    return advection_table(key)


def draw_inverse_x(key, part):
    return block_inverse(key, 0, CX)


def draw_inverse_y(key, part):
    return block_inverse(key, 1, CY)


def draw_inverse_z(key, part):
    return block_inverse(key, 2, CZ)


def draw_reduced_x(key, part):
    return reduced_inverse(key, 0, CX, NX // CX)


def draw_reduced_y(key, part):
    return reduced_inverse(key, 1, CY, NY // CY)


def draw_reduced_z(key, part):
    return reduced_inverse(key, 2, CZ, NZ // CZ)


def setup_inputs(seed: int = 0) -> dict:
    arg_keys = jax.random.split(jax.random.key(seed), 9)
    return {
        "flow_state": draw_flow_state(jax.random.fold_in(arg_keys[8], 71), 0),
        "advection": draw_advection(jax.random.fold_in(arg_keys[8], 71), 0),
        "inverse_x": draw_inverse_x(jax.random.fold_in(arg_keys[8], 71), 0),
        "inverse_y": draw_inverse_y(jax.random.fold_in(arg_keys[8], 71), 0),
        "inverse_z": draw_inverse_z(jax.random.fold_in(arg_keys[8], 71), 0),
        "reduced_x": draw_reduced_x(jax.random.fold_in(arg_keys[8], 71), 0),
        "reduced_y": draw_reduced_y(jax.random.fold_in(arg_keys[8], 71), 0),
        "reduced_z": draw_reduced_z(jax.random.fold_in(arg_keys[8], 71), 0),
    }


exact_mode = lax.Precision.HIGHEST
gas_ratio = 0.4
courant = 8000.0
damping = 0.0625
fourth_coef = 0.5

def primitives(flow_state):
    density = flow_state[0]
    velocity = flow_state[1:4] / density
    kinetic = 0.5 * lax.optimization_barrier(jnp.sum(velocity * velocity, axis=0))
    internal = jnp.maximum(flow_state[4] / density - kinetic, 0.25)
    pressure = gas_ratio * density * internal
    return (velocity, internal, pressure)

def flux_component(flow_state, velocity, pressure, variable, direction):
    carried = velocity[direction]
    if variable == 0:
        return flow_state[1 + direction]
    if variable < 4:
        moment = flow_state[variable] * carried
        if variable - 1 == direction:
            moment = moment + pressure
        return moment
    return (flow_state[4] + pressure) * carried

def residual_field(flow_state, velocity, pressure):
    collected = []
    for variable in range(VARS):
        field = flow_state[variable]
        running = jnp.zeros_like(field)
        for direction in range(3):
            line_axis = 2 - direction
            flux = flux_component(flow_state, velocity, pressure, variable, direction)
            running = running - 0.5 * (jnp.roll(flux, -1, line_axis) - jnp.roll(flux, 1, line_axis))
            fourth = jnp.roll(field, 2, line_axis) - 4.0 * jnp.roll(field, 1, line_axis) + 6.0 * field - 4.0 * jnp.roll(field, -1, line_axis) + jnp.roll(field, -2, line_axis)
            running = running - damping * fourth
        collected.append(running)
    return jnp.stack(collected)

def neighbour_table(reduced):
    blocks = reduced.shape[0] // 4
    padded = jnp.pad(reduced, ((2, 2), (0, 0)))
    picked = (4 * np.arange(blocks)[:, None] + np.array([0, 1, 6, 7])[None, :]).reshape(-1)
    return padded[picked]

def line_solve(line_field, line_axis, inverse, reduced, speed):
    moved = jnp.moveaxis(line_field, line_axis, -1)
    block_len = inverse.shape[0]
    blocks = reduced.shape[0] // 4
    leading = moved.shape[:-1]
    split = moved.reshape(leading + (blocks, block_len))
    local_part = jnp.einsum('ij,abpj->abpi', inverse, split, precision=exact_mode)
    boundary = jnp.stack([local_part[..., 0], local_part[..., 1], local_part[..., block_len - 2], local_part[..., block_len - 1]], axis=-1).reshape(leading + (4 * blocks,))
    nearby = jnp.einsum('rq,abq->abr', neighbour_table(reduced), boundary, precision=exact_mode).reshape(leading + (blocks, 4))
    lower_one = -0.5 * speed - 4.0 * fourth_coef
    upper_one = 0.5 * speed - 4.0 * fourth_coef
    left_first = fourth_coef * nearby[..., 0] + lower_one * nearby[..., 1]
    left_second = fourth_coef * nearby[..., 1]
    right_first = fourth_coef * nearby[..., 2]
    right_second = upper_one * nearby[..., 2] + fourth_coef * nearby[..., 3]
    correction = inverse[:, 0] * left_first[..., None] + inverse[:, 1] * left_second[..., None] + inverse[:, block_len - 2] * right_first[..., None] + inverse[:, block_len - 1] * right_second[..., None]
    solved = (local_part - correction).reshape(moved.shape)
    return jnp.moveaxis(solved, -1, line_axis)

def reference(flow_state, advection, inverse_x, inverse_y, inverse_z, reduced_x, reduced_y, reduced_z):
    velocity, internal, pressure = primitives(flow_state)
    wave_speed = lax.optimization_barrier(jnp.sum(jnp.abs(velocity), axis=0)) + jnp.sqrt(3.0 * 1.4 * gas_ratio * internal)
    top_speed = jnp.max(wave_speed)
    time_step = courant / top_speed
    residual = residual_field(flow_state, velocity, pressure)
    rms_norm = jnp.sqrt(lax.optimization_barrier(jnp.sum(residual * residual, axis=(1, 2, 3))) / (NX * NY * NZ))
    inverses = (inverse_x, inverse_y, inverse_z)
    reduceds = (reduced_x, reduced_y, reduced_z)
    collected = []
    for variable in range(VARS):
        line_field = time_step * residual[variable]
        for direction in range(3):
            line_field = line_solve(line_field, 2 - direction, inverses[direction][variable], reduceds[direction][variable], advection[direction, variable])
        collected.append(line_field)
    return (jnp.stack(collected), rms_norm)
```

```python
import functools

import jax
import jax.numpy as jnp
from jax import lax
from jax.experimental import pallas as pl
from jax.experimental.pallas import tpu as pltpu
from jax.sharding import PartitionSpec as P

MESH = pl.DeviceIdType.MESH
HIGHEST = lax.Precision.HIGHEST
gas_ratio = 0.4
courant = 8000.0
damping = 0.0625
fourth_coef = 0.5
AXES = ("gx", "gy", "gz")
f32 = jnp.float32
bf16 = jnp.bfloat16

NN = (((1,), (0,)), ((), ()))
NT = (((1,), (1,)), ((), ()))
TN = (((0,), (0,)), ((), ()))


def exact_dot(a, b, dims=NN):
    return lax.dot_general(a, b, dims, precision=HIGHEST, preferred_element_type=f32)


def one_dot(a, b, dims=NN):
    return lax.dot_general(a, b, dims, preferred_element_type=f32)


def halves(a):
    high = a.astype(bf16)
    low = (a - high.astype(f32)).astype(bf16)
    return high, low


def split_dot(a, b, dims=NN):
    return one_dot(a[0], b[0], dims) + (one_dot(a[0], b[1], dims) + one_dot(a[1], b[0], dims))


def stack3(a):
    high, low = halves(a)
    return jnp.concatenate([high, low, high], axis=0)


def iota(shape, dim):
    return lax.broadcasted_iota(jnp.int32, shape, dim)


def ones_where(mask):
    return jnp.where(mask, 1.0, 0.0).astype(f32)


def primitives(u):
    inverse = 1.0 / u[0]
    velocity = [u[1] * inverse, u[2] * inverse, u[3] * inverse]
    kinetic = 0.5 * (velocity[0] * velocity[0] + velocity[1] * velocity[1] + velocity[2] * velocity[2])
    internal = jnp.maximum(u[4] * inverse - kinetic, 0.25)
    pressure = gas_ratio * u[0] * internal
    return velocity, internal, pressure


def fluxes(u, direction, values=None):
    velocity, internal, pressure = primitives(u) if values is None else values
    carried = velocity[direction]
    found = [u[1 + direction]]
    for component in range(3):
        moment = u[1 + component] * carried
        if component == direction:
            moment = moment + pressure
        found.append(moment)
    found.append((u[4] + pressure) * carried)
    return found


def coupled(col, block, part, speed):
    lower = -0.5 * speed - 4.0 * fourth_coef
    upper = 0.5 * speed - 4.0 * fourth_coef
    value = jnp.where((part == 0) & (col == 4 * block - 2), fourth_coef, 0.0)
    value = jnp.where((part == 0) & (col == 4 * block - 1), lower, value)
    value = jnp.where((part == 1) & (col == 4 * block - 1), fourth_coef, value)
    value = jnp.where((part == 2) & (col == 4 * block + 4), fourth_coef, value)
    value = jnp.where((part == 3) & (col == 4 * block + 4), upper, value)
    return jnp.where((part == 3) & (col == 4 * block + 5), fourth_coef, value).astype(f32)


def face_pick(shape, size, row_dim=0):
    r, c = iota(shape, row_dim), iota(shape, 1 - row_dim)
    return ones_where((r < 4) & (c == jnp.where(r < 2, r, size - 4 + r)))


def kernel(dims, state_h, adv_h, ax_h, ay_h, az_h, rx_h, ry_h, rz_h, out, stats_out,
           uz, uy, hx, res, edge, field, first, ext, wyh, wyl, wts, pts, pto, khi, klo, azx, kue, mb, cxf,
           xb, ysend, yrecv, zsend, zrecv, esend, erecv, stx, sty, stz,
           ax, ay, az, rx, ry, rz, adv,
           in_sem, aux_sem, halo_send, halo_recv, xs, xr, ys, yr, zs, zr, es, er, ss, sr):
    counts, nv, cz, cy, cx, cells = dims
    gx, gy, gz = counts
    rows = cz * cy
    pack = xb.shape[1]
    nc = 2 if gy == 2 else 4
    plane4 = 4 * cy
    me = [lax.axis_index(axis) for axis in AXES]

    loads = []
    for v in range(nv):
        copy = pltpu.make_async_copy(state_h.at[v], uz.at[v, pl.ds(2 * cy, rows)], in_sem.at[v])
        copy.start()
        loads.append(copy)
    aux = []
    for i, (src, dst) in enumerate([(az_h, az), (ay_h, ay), (ry_h, ry), (rz_h, rz), (rx_h, rx), (adv_h, adv), (ax_h, ax)]):
        copy = pltpu.make_async_copy(src, dst, aux_sem.at[i])
        copy.start()
        aux.append(copy)

    barrier = pltpu.get_barrier_semaphore()
    total = 0
    for axis, count, place in zip(AXES, counts, me):
        for k in range(1, count):
            pl.semaphore_signal(barrier, inc=1, device_id={axis: lax.rem(place + k, count)}, device_id_type=MESH)
            total += 1
    for copy in loads:
        copy.wait()

    lane_c = iota((rows, cx), 1)

    def faces_to_rows(load):
        packed = jnp.zeros((rows, cx), f32)
        for v in range(nv):
            moved = pltpu.roll(load(v), 4 * v + 2, 1)
            packed = jnp.where(lane_c // 4 == v, moved, packed)
        return jnp.transpose(packed)[0:pack]

    hx[0] = faces_to_rows(lambda v: uz[v, pl.ds(2 * cy, rows), :])
    pl.semaphore_wait(barrier, total)

    def ring(axis, slot, down_src, down_dst, up_src, up_dst, far_first=False):
        count, place = counts[axis], me[axis]
        lower = lax.rem(place + count - 1, count)
        upper = lax.rem(place + 1, count)
        down = pltpu.make_async_remote_copy(
            src_ref=down_src, dst_ref=down_dst, send_sem=halo_send.at[slot], recv_sem=halo_recv.at[slot],
            device_id={AXES[axis]: lower}, device_id_type=MESH)
        up = pltpu.make_async_remote_copy(
            src_ref=up_src, dst_ref=up_dst, send_sem=halo_send.at[slot + 1], recv_sem=halo_recv.at[slot + 1],
            device_id={AXES[axis]: upper}, device_id_type=MESH)
        if far_first:
            @pl.when(place == count - 1)
            def _():
                up.start()
                down.start()

            @pl.when(place < count - 1)
            def _():
                down.start()
                up.start()
        else:
            down.start()
            up.start()
        return [down, up]

    def spread(axis, src, dst, send, recv):
        count, place = counts[axis], me[axis]
        copies = []
        for k in range(1, count):
            target = lax.rem(place + k, count)
            copy = pltpu.make_async_remote_copy(
                src_ref=src(target), dst_ref=dst, send_sem=send(k - 1), recv_sem=recv(k - 1),
                device_id={AXES[axis]: target}, device_id_type=MESH)
            copy.start()
            copies.append(copy)
        return copies

    z_halo = ring(2, 4,
                  uz.at[:, pl.ds(2 * cy, 2 * cy)], uz.at[:, pl.ds((cz + 2) * cy, 2 * cy)],
                  uz.at[:, pl.ds(cz * cy, 2 * cy)], uz.at[:, pl.ds(0, 2 * cy)], far_first=True)
    x_halo = ring(0, 0, hx.at[0], hx.at[1], hx.at[0], hx.at[2])

    for v in range(nv):
        for y in range(cy):
            uy[v, pl.ds((y + 2) * cz, cz), :] = uz[v, pl.ds(2 * cy + y, cz, stride=cy), :]
    y_halo = ring(1, 2,
                  uy.at[:, pl.ds(2 * cz, 2 * cz)], uy.at[:, pl.ds((cy + 2) * cz, 2 * cz)],
                  uy.at[:, pl.ds(cy * cz, 2 * cz)], uy.at[:, pl.ds(0, 2 * cz)])

    for copy in aux:
        copy.wait()

    spread_z = ones_where(iota((cz, rows), 1) // cy == iota((cz, rows), 0))
    spread_y = ones_where(lax.rem(iota((cy, rows), 1), cy) == iota((cy, rows), 0))
    for v in range(nv):
        azx[...] = exact_dot(az[v], spread_z)
        wide_y = exact_dot(ay[v], spread_y)

        @pl.loop(0, cz)
        def _(z):
            high, low = halves(azx[pl.ds(z, 1), :] * wide_y)
            at = pl.ds(pl.multiple_of(z * cy, cy), cy)
            khi[v, at, :] = high
            klo[v, at, :] = low

    nd = wyh.shape[1] // cz
    row_y, col_y = iota((nd, 4 * gy), 0), iota((nd, 4 * gy), 1)
    block_y = row_y // nc
    part_y = row_y % nc + (jnp.where(block_y == 0, 2, 0) if nc == 2 else 0)
    pick_y = iota((4 * gy, 8), 0)
    pick_y = ones_where((pick_y == 4 * me[1] + iota((4 * gy, 8), 1)) & (iota((4 * gy, 8), 1) < 4))
    same_z = iota((cz, rows), 1) // cy == iota((cz, rows), 0)
    for v in range(nv):
        response = exact_dot(exact_dot(ry[v], pick_y), exact_dot(face_pick((8, cy), cy), ay[v]))
        wide = exact_dot(exact_dot(coupled(col_y, block_y, part_y, adv[1, v]), response), spread_y)
        for n in range(nd):
            high, low = halves(jnp.where(same_z, wide[n:n + 1, :], 0.0))
            wyh[v, pl.ds(n * cz, cz), :] = high
            wyl[v, pl.ds(n * cz, cz), :] = low

    nz = wts.shape[1] // cy
    row_z, col_z = iota((nz, 4 * gz), 0), iota((nz, 4 * gz), 1)
    dest = row_z // 2
    wanted = jnp.where(dest > me[2], 4 * dest - 2, 4 * dest + 4) + row_z % 2
    sel_z = ones_where((dest != me[2]) & (col_z == wanted) & (dest < gz))
    pick_z = ones_where((iota((4 * gz, 8), 0) == 4 * me[2] + iota((4 * gz, 8), 1)) & (iota((4 * gz, 8), 1) < 4))
    width = wts.shape[2]
    tiled = ones_where(lax.rem(iota((8, width), 1), plane4) // cy == iota((8, width), 0))
    low_lane = iota((1, width), 1) >= 2 * plane4
    same_y = lax.rem(iota((cy, width), 1), cy) == iota((cy, width), 0)

    def stacked(a):
        high = a.astype(bf16).astype(f32)
        return jnp.where(low_lane, a - high, high)

    for v in range(nv):
        given = stacked(exact_dot(exact_dot(sel_z, exact_dot(rz[v], pick_z)), tiled))
        for n in range(nz):
            wts[v, pl.ds(n * cy, cy), :] = jnp.where(same_y, given[n:n + 1, :], 0.0).astype(bf16)

    def part(u, direction):
        ahead = fluxes(u[1], direction)
        behind = fluxes(u[-1], direction)
        found = []
        for v in range(nv):
            fourth = u[-2][v] - 4.0 * u[-1][v] + 6.0 * u[0][v] - 4.0 * u[1][v] + u[2][v]
            found.append(-0.5 * (ahead[v] - behind[v]) - damping * fourth)
        return found

    for copy in y_halo:
        copy.wait_recv()

    @pl.loop(0, cy)
    def _(y):
        u = {}
        for off in range(-2, 3):
            at = pl.ds(pl.multiple_of((y + 2 + off) * cz, cz), cz)
            u[off] = [uy[v, at, :] for v in range(nv)]
        found = part(u, 1)
        for v in range(nv):
            res[v, pl.ds(y, cz, stride=cy), :] = found[v]

    for copy in x_halo:
        copy.wait_recv()
    sub4 = iota((4, rows), 0)
    merged = [jnp.where(sub4 < 2, hx[2, 4 * v:4 * v + 4, :], hx[1, 4 * v:4 * v + 4, :]) for v in range(nv)]
    halo_flux = fluxes(merged, 0)
    sub8, lane8 = iota((8, cx), 0), iota((8, cx), 1)

    def at_lane(row, lane, value):
        return jnp.where((sub8 == row) & (lane8 == lane), value, 0.0)

    weights = (at_lane(0, 0, -damping) + at_lane(1, 0, 4.0 * damping) + at_lane(1, 1, -damping)
               + at_lane(2, cx - 2, -damping) + at_lane(2, cx - 1, 4.0 * damping) + at_lane(3, cx - 1, -damping)
               + at_lane(6, cx - 1, -0.5) + at_lane(5, 0, 0.5)).astype(bf16)
    weights = jnp.concatenate([weights, weights], axis=0)
    weights = jnp.concatenate([weights, weights], axis=0)
    for v in range(nv):
        both = jnp.concatenate([merged[v], halo_flux[v]], axis=0)
        high = both.astype(bf16).astype(f32)
        mid = (both - high).astype(bf16).astype(f32)
        parts = jnp.concatenate([high, mid, both - high - mid, jnp.zeros_like(both)], axis=0).astype(bf16)
        edge[v] = one_dot(parts, weights, TN)

    step = 2 * cy
    lane = iota((step, cx), 1)

    def shifted(a, offset):
        moved = pltpu.roll(a, (-offset) % cx, 1)
        inside = lane < cx - offset if offset > 0 else lane >= -offset
        return jnp.where(inside, moved, 0.0)

    def body(i, carry):
        squares, top = carry
        base = pl.multiple_of(i * step, step)
        u = {}
        for off in range(-2, 3):
            at = pl.ds(pl.multiple_of(base + (off + 2) * cy, cy), step)
            u[off] = [uz[v, at, :] for v in range(nv)]
        found = part(u, 2)
        values = primitives(u[0])
        velocity, internal, _ = values
        wave = (jnp.abs(velocity[0]) + jnp.abs(velocity[1]) + jnp.abs(velocity[2])
                + jnp.sqrt(3.0 * 1.4 * gas_ratio * internal))
        top = jnp.maximum(top, wave)
        flux_x = fluxes(u[0], 0, values)
        new_squares = []
        for v in range(nv):
            c = u[0][v]
            fourth = (shifted(c, -2) + shifted(c, 2)) - 4.0 * (shifted(c, -1) + shifted(c, 1)) + 6.0 * c
            along_x = -0.5 * (shifted(flux_x[v], 1) - shifted(flux_x[v], -1)) - damping * fourth
            at = pl.ds(base, step)
            value = res[v, at, :] + found[v] + (along_x + edge[v, at, :])
            res[v, at, :] = value
            new_squares.append(squares[v] + value * value)
        return tuple(new_squares), top

    zero = jnp.zeros((step, cx), f32)
    last = cz // 2 - 1
    carry = lax.fori_loop(1, last, body, ((zero,) * nv, zero))
    for copy in z_halo:
        copy.wait_recv()
    squares, top = lax.fori_loop(0, 2, lambda j, c: body(j * last, c), carry)

    y_copies = []
    for v in range(nv):
        inner = split_dot(halves(res[v]), halves(ax[v]), NT)
        first[v] = inner
        ysend[v] = split_dot((wyh[v], wyl[v]), halves(inner))[0:gy * nc * cz].reshape(gy, nc * cz, cx)
        y_copies.append(spread(1, lambda t: ysend.at[v, t], yrecv.at[v, me[1]],
                               lambda k: ys.at[v, k], lambda k: yr.at[v, k]))

    sub_s = iota((8, cx), 0)
    tile = jnp.where(sub_s == 5, jnp.max(top, axis=0, keepdims=True), 0.0)
    for v in range(nv):
        tile = jnp.where(sub_s == v, jnp.sum(squares[v], axis=0, keepdims=True), tile)
    sty[me[1]] = tile
    stat_copies = [spread(1, lambda t: sty.at[me[1]], sty.at[me[1]], lambda k: ss.at[0, k], lambda k: sr.at[0, k])]

    def gathered(ref, count):
        result = ref[0]
        for q in range(1, count):
            result = jnp.where(sub_s < nv, result + ref[q], jnp.maximum(result, ref[q]))
        return result

    def end_planes(ref, v):
        return jnp.concatenate([ref[v, pl.ds(0, 2 * cy), :], ref[v, pl.ds((cz - 2) * cy, 2 * cy), :]], axis=0)

    z_copies = []
    for v in range(nv):
        for copy in y_copies[v]:
            copy.wait_recv()
        taken = ysend[v, me[1]]
        for k in range(1, gy):
            taken = taken + yrecv[v, lax.rem(me[1] + k, gy)]
        start = jnp.where(me[1] == 0, cy - 2, 0)
        for c in range(nc):
            at = pl.ds(start + c, cz, stride=cy) if nc == 2 else pl.ds(c if c < 2 else cy - 4 + c, cz, stride=cy)
            first[v, at, :] = first[v, at, :] - taken[c * cz:(c + 1) * cz]
        field[v] = split_dot((khi[v], klo[v]), halves(first[v]))
        zsend[v] = one_dot(wts[v], stack3(end_planes(field, v)))[0:gz * 2 * cy].reshape(gz, 2 * cy, cx)
        z_copies.append(spread(2, lambda t: zsend.at[v, t], zrecv.at[v, me[2]],
                               lambda k: zs.at[v, k], lambda k: zr.at[v, k]))

    xb[me[0]] = faces_to_rows(lambda v: field[v])
    x_copies = [spread(0, lambda t: xb.at[me[0]], xb.at[me[0]], lambda k: xs.at[k], lambda k: xr.at[k])]
    for copy in stat_copies[0]:
        copy.wait_recv()
    stx[me[0]] = gathered(sty, gy)
    stat_copies.append(spread(0, lambda t: stx.at[me[0]], stx.at[me[0]], lambda k: ss.at[1, k], lambda k: sr.at[1, k]))

    mb[...] = jnp.zeros_like(mb)
    cxf[...] = jnp.zeros_like(cxf)
    wide_x = gx * pack
    in_x = lax.rem(iota((4 * gx, wide_x), 1), pack)
    block_x = iota((4 * gx, wide_x), 1) // pack
    row_x = iota((8, 4 * gx), 0)
    for v in range(nv):
        m = exact_dot(coupled(iota((8, 4 * gx), 1), me[0], row_x, adv[0, v]), rx[v])
        to_pack = ones_where((in_x // 4 == v) & (iota((4 * gx, wide_x), 0) == 4 * block_x + lax.rem(in_x + 2, 4)))
        placed = exact_dot(m, to_pack)
        columns = exact_dot(face_pick((8, cx), cx), ax[v], NT)
        high = columns.astype(bf16).astype(f32)
        for k in range(3):
            at = pl.ds(4 * v + 32 * k, 4)
            mb[at, :] = placed[0:4]
            cxf[at, v * cx:(v + 1) * cx] = (high if k < 2 else columns - high)[0:4]

    row_l, col_l = iota((8, 4 * gz), 0), iota((8, 4 * gz), 1)
    sel_lf = ones_where((row_l < 4) & (col_l == 4 * me[2] + jnp.where(row_l < 2, row_l - 2, row_l + 2)))
    r8, c8 = iota((8, 8), 0), iota((8, 8), 1)
    for v in range(nv):
        near = exact_dot(sel_lf, rz[v])
        square = exact_dot(near, sel_lf, NT)

        def e(i, j):
            return square[i:i + 1, j:j + 1]

        det_l = e(0, 0) * e(1, 1) - e(0, 1) * e(1, 0)
        det_f = e(2, 2) * e(3, 3) - e(2, 3) * e(3, 2)
        inv_l = 1.0 / jnp.where(me[2] > 0, det_l, 1.0)
        inv_f = 1.0 / jnp.where(me[2] < gz - 1, det_f, 1.0)
        mix = ones_where((r8 == c8) & (r8 < 4))
        for i in range(2):
            for j, value in enumerate([(e(2 + i, 0) * e(1, 1) - e(2 + i, 1) * e(1, 0)) * inv_l,
                                       (e(2 + i, 1) * e(0, 0) - e(2 + i, 0) * e(0, 1)) * inv_l]):
                mix = jnp.where((r8 == 2 + i) & (c8 == j), value, mix)
            for j, value in enumerate([(e(i, 2) * e(3, 3) - e(i, 3) * e(3, 2)) * inv_f,
                                       (e(i, 3) * e(2, 2) - e(i, 2) * e(2, 3)) * inv_f]):
                mix = jnp.where((r8 == i) & (c8 == 2 + j), value, mix)
        speed = adv[2, v]
        weigh = jnp.where((r8 == c8) & (r8 < 4), fourth_coef, 0.0)
        weigh = jnp.where((r8 == 0) & (c8 == 1), -0.5 * speed - 4.0 * fourth_coef, weigh)
        weigh = jnp.where((r8 == 3) & (c8 == 2), 0.5 * speed - 4.0 * fourth_coef, weigh).astype(f32)
        columns = exact_dot(az[v], face_pick((8, cz), cz), NT)
        peers = exact_dot(weigh, mix)
        own = exact_dot(weigh, exact_dot(near, pick_z))
        kue[v, 0] = stacked(exact_dot(exact_dot(columns, peers), tiled))
        kue[v, 1] = stacked(exact_dot(exact_dot(columns, own), tiled))

    @pl.loop(0, cz)
    def _(z):
        at = pl.ds(pl.multiple_of(z * cy, cy), cy)
        for v in range(nv):
            pts[v, at, :] = jnp.where(same_y, kue[v, 0, pl.ds(z, 1), :], 0.0).astype(bf16)
            pto[v, at, :] = jnp.where(same_y, kue[v, 1, pl.ds(z, 1), :], 0.0).astype(bf16)

    for v in range(nv):
        field[v] = field[v] - one_dot(pto[v], stack3(end_planes(field, v)))

    for group in x_copies + [stat_copies[1]]:
        for copy in group:
            copy.wait_recv()
    stz[me[2]] = gathered(stx, gx)
    stat_copies.append(spread(2, lambda t: stz.at[me[2]], stz.at[me[2]], lambda k: ss.at[2, k], lambda k: sr.at[2, k]))

    ext[...] = jnp.transpose(split_dot(halves(mb[...]), halves(xb[...].reshape(wide_x, rows))))
    lane_e = iota((plane4, cx), 1)
    lane_v = jnp.where(lane_e < 96, (lane_e % 32) // 4, -1)
    ends = jnp.concatenate([ext[pl.ds(0, 2 * cy), :], ext[pl.ds((cz - 2) * cy, 2 * cy), :]], axis=0)

    def by_variable(table, a):
        result = None
        for v in range(nv):
            term = one_dot(table[v], stack3(jnp.where(lane_v == v, a, 0.0)))
            result = term if result is None else result + term
        return result

    esend[...] = by_variable(wts, ends)[0:gz * 2 * cy].reshape(gz, 2 * cy, cx)
    e_copies = spread(2, lambda t: esend.at[t], erecv.at[me[2]], lambda k: es.at[k], lambda k: er.at[k])
    ext[...] = ext[...] - by_variable(pto, ends)

    def sides(load):
        before, after = None, None
        for k in range(1, gz):
            q = lax.rem(me[2] + k, gz)
            value = load(q)
            left, right = jnp.where(q < me[2], value, 0.0), jnp.where(q > me[2], value, 0.0)
            before = left if before is None else before + left
            after = right if after is None else after + right
        return jnp.concatenate([before, after], axis=0)

    for v in range(nv):
        for copy in z_copies[v]:
            copy.wait_recv()
        field[v] = field[v] - one_dot(pts[v], stack3(sides(lambda q: zrecv[v, q])))

    for copy in stat_copies[2]:
        copy.wait_recv()
    final = gathered(stz, gz)
    norm = jnp.sqrt(jnp.sum(final, axis=1, keepdims=True) / float(cells))
    fastest = courant / jnp.max(final, axis=1, keepdims=True)
    stats_out[...] = jnp.broadcast_to(norm, (8, cx))
    time_step = fastest[5:6, :]

    for copy in e_copies:
        copy.wait_recv()
    solved = ext[...] - by_variable(pts, sides(lambda q: erecv[q]))
    high = solved.astype(bf16).astype(f32)
    parts = jnp.where((lane_c >= 32) & (lane_c < 64), solved - high, high).astype(bf16)
    for v in range(nv):
        out[v] = (field[v] - one_dot(parts, cxf[:, v * cx:(v + 1) * cx].astype(bf16))) * time_step

    for group in [x_halo, y_halo, z_halo, e_copies] + x_copies + y_copies + z_copies + stat_copies:
        for copy in group:
            copy.wait_send()


def finish(nv, solved, stats, update, norm, sem):
    copies = []
    for v in range(nv):
        copy = pltpu.make_async_copy(solved.at[v], update.at[v], sem.at[v])
        copy.start()
        copies.append(copy)
    for v in range(nv):
        norm[v] = stats[v, 0]
    for copy in copies:
        copy.wait()


def shards(counts, flow_state, advection, inverse_x, inverse_y, inverse_z, reduced_x, reduced_y, reduced_z):
    nv, cz, cy, cx = flow_state.shape
    gx, gy, gz = counts
    rows = cz * cy
    cells = rows * cx * gx * gy * gz
    most = max(counts) - 1
    hbm = pl.BlockSpec(memory_space=pltpu.HBM)
    vmem = pl.BlockSpec(memory_space=pltpu.VMEM)
    dma = pltpu.SemaphoreType.DMA
    pack = -(-4 * nv // 8) * 8
    nc = 2 if gy == 2 else 4
    nd = max(8, gy * nc)
    nz = max(8, 2 * gz)
    width = 12 * cy
    out, stats = pl.pallas_call(
        functools.partial(kernel, (counts, nv, cz, cy, cx, cells)),
        out_shape=(pltpu.VMEM((nv, rows, cx), f32), pltpu.VMEM((8, cx), f32)),
        in_specs=[hbm] * 8,
        out_specs=(vmem, vmem),
        scratch_shapes=[
            pltpu.VMEM((nv, (cz + 4) * cy, cx), f32),
            pltpu.VMEM((nv, (cy + 4) * cz, cx), f32),
            pltpu.VMEM((3, pack, rows), f32),
            pltpu.VMEM((nv, rows, cx), f32),
            pltpu.VMEM((nv, rows, cx), f32),
            pltpu.VMEM((nv, rows, cx), f32),
            pltpu.VMEM((nv, rows, cx), f32),
            pltpu.VMEM((rows, cx), f32),
            pltpu.VMEM((nv, nd * cz, rows), bf16),
            pltpu.VMEM((nv, nd * cz, rows), bf16),
            pltpu.VMEM((nv, nz * cy, width), bf16),
            pltpu.VMEM((nv, rows, width), bf16),
            pltpu.VMEM((nv, rows, width), bf16),
            pltpu.VMEM((nv, rows, rows), bf16),
            pltpu.VMEM((nv, rows, rows), bf16),
            pltpu.VMEM((cz, rows), f32),
            pltpu.VMEM((nv, 2, cz, width), f32),
            pltpu.VMEM((cx, gx * pack), f32),
            pltpu.VMEM((cx, nv * cx), f32),
            pltpu.VMEM((gx, pack, rows), f32),
            pltpu.VMEM((nv, gy, nc * cz, cx), f32),
            pltpu.VMEM((nv, gy, nc * cz, cx), f32),
            pltpu.VMEM((nv, gz, 2 * cy, cx), f32),
            pltpu.VMEM((nv, gz, 2 * cy, cx), f32),
            pltpu.VMEM((gz, 2 * cy, cx), f32),
            pltpu.VMEM((gz, 2 * cy, cx), f32),
            pltpu.VMEM((gx, 8, cx), f32),
            pltpu.VMEM((gy, 8, cx), f32),
            pltpu.VMEM((gz, 8, cx), f32),
            pltpu.VMEM(inverse_x.shape, f32),
            pltpu.VMEM(inverse_y.shape, f32),
            pltpu.VMEM(inverse_z.shape, f32),
            pltpu.VMEM(reduced_x.shape, f32),
            pltpu.VMEM(reduced_y.shape, f32),
            pltpu.VMEM(reduced_z.shape, f32),
            pltpu.SMEM(advection.shape, f32),
            dma((nv,)),
            dma((7,)),
            dma((6,)), dma((6,)),
            dma((gx - 1,)), dma((gx - 1,)),
            dma((nv, gy - 1)), dma((nv, gy - 1)),
            dma((nv, gz - 1)), dma((nv, gz - 1)),
            dma((gz - 1,)), dma((gz - 1,)),
            dma((3, most)), dma((3, most)),
        ],
        compiler_params=pltpu.CompilerParams(
            collective_id=0, has_side_effects=True, vmem_limit_bytes=60 * 1024 * 1024),
    )(flow_state.reshape(nv, rows, cx), advection, inverse_x, inverse_y, inverse_z, reduced_x, reduced_y, reduced_z)
    update, norm = pl.pallas_call(
        functools.partial(finish, nv),
        out_shape=(jax.ShapeDtypeStruct((nv, rows, cx), f32), jax.ShapeDtypeStruct((nv,), f32)),
        in_specs=[vmem, vmem],
        out_specs=(pl.BlockSpec(memory_space=pltpu.HBM), pl.BlockSpec(memory_space=pltpu.SMEM)),
        scratch_shapes=[dma((nv,))],
        compiler_params=pltpu.CompilerParams(vmem_limit_bytes=4 * 1024 * 1024),
    )(out, stats)
    return update.reshape(flow_state.shape), norm


def solution(mesh):
    counts = tuple(mesh.shape[axis] for axis in AXES)
    placed = (P(None, "gz", "gy", "gx"), P(), P(), P(), P(), P(), P(), P())
    return jax.shard_map(
        functools.partial(shards, counts),
        mesh=mesh,
        in_specs=placed,
        out_specs=(P(None, "gz", "gy", "gx"), P()),
        check_vma=False,
    )
```

```python
import functools

import jax
import jax.numpy as jnp
from jax import lax
from jax.experimental import pallas as pl
from jax.experimental.pallas import tpu as pltpu
from jax.sharding import PartitionSpec as P

MESH = pl.DeviceIdType.MESH
HIGHEST = lax.Precision.HIGHEST
gas_ratio = 0.4
courant = 8000.0
damping = 0.0625
fourth_coef = 0.5
AXES = ("gx", "gy", "gz")
f32 = jnp.float32
bf16 = jnp.bfloat16

NN = (((1,), (0,)), ((), ()))
NT = (((1,), (1,)), ((), ()))
TN = (((0,), (0,)), ((), ()))


def exact_dot(a, b, dims=NN):
    return lax.dot_general(a, b, dims, precision=HIGHEST, preferred_element_type=f32)


def one_dot(a, b, dims=NN):
    return lax.dot_general(a, b, dims, preferred_element_type=f32)


def halves(a):
    high = a.astype(bf16)
    low = (a - high.astype(f32)).astype(bf16)
    return high, low


def split_dot(a, b, dims=NN):
    return one_dot(a[0], b[0], dims) + (one_dot(a[0], b[1], dims) + one_dot(a[1], b[0], dims))


def stack3(a):
    high, low = halves(a)
    return jnp.concatenate([high, low, high], axis=0)


def iota(shape, dim):
    return lax.broadcasted_iota(jnp.int32, shape, dim)


def ones_where(mask):
    return jnp.where(mask, 1.0, 0.0).astype(f32)


def primitives(u):
    inverse = 1.0 / u[0]
    velocity = [u[1] * inverse, u[2] * inverse, u[3] * inverse]
    kinetic = 0.5 * (velocity[0] * velocity[0] + velocity[1] * velocity[1] + velocity[2] * velocity[2])
    internal = jnp.maximum(u[4] * inverse - kinetic, 0.25)
    pressure = gas_ratio * u[0] * internal
    return velocity, internal, pressure


def fluxes(u, direction, values=None):
    velocity, internal, pressure = primitives(u) if values is None else values
    carried = velocity[direction]
    found = [u[1 + direction]]
    for component in range(3):
        moment = u[1 + component] * carried
        if component == direction:
            moment = moment + pressure
        found.append(moment)
    found.append((u[4] + pressure) * carried)
    return found


def coupled(col, block, part, speed):
    lower = -0.5 * speed - 4.0 * fourth_coef
    upper = 0.5 * speed - 4.0 * fourth_coef
    value = jnp.where((part == 0) & (col == 4 * block - 2), fourth_coef, 0.0)
    value = jnp.where((part == 0) & (col == 4 * block - 1), lower, value)
    value = jnp.where((part == 1) & (col == 4 * block - 1), fourth_coef, value)
    value = jnp.where((part == 2) & (col == 4 * block + 4), fourth_coef, value)
    value = jnp.where((part == 3) & (col == 4 * block + 4), upper, value)
    return jnp.where((part == 3) & (col == 4 * block + 5), fourth_coef, value).astype(f32)


def face_pick(shape, size, row_dim=0):
    r, c = iota(shape, row_dim), iota(shape, 1 - row_dim)
    return ones_where((r < 4) & (c == jnp.where(r < 2, r, size - 4 + r)))


def kernel(dims, state_h, adv_h, ax_h, ay_h, az_h, rx_h, ry_h, rz_h, out, stats_out,
           uz, uy, hx, res, edge, field, first, ext, wys, wts, pts, pto, kzh, kzl, kyh, kyl, axs, cyt, mb, cxf,
           xb, ysend, yrecv, zsend, zrecv, esend, erecv, stx, sty, stz,
           ax, ay, az, rx, ry, rz, adv,
           in_sem, aux_sem, halo_send, halo_recv, xs, xr, ys, yr, zs, zr, es, er, ss, sr):
    counts, nv, cz, cy, cx, cells = dims
    gx, gy, gz = counts
    rows = cz * cy
    pack = xb.shape[1]
    nc = 2 if gy == 2 else 4
    plane4 = 4 * cy
    me = [lax.axis_index(axis) for axis in AXES]

    loads = []
    for v in range(nv):
        copy = pltpu.make_async_copy(state_h.at[v], uz.at[v, pl.ds(2 * cy, rows)], in_sem.at[v])
        copy.start()
        loads.append(copy)
    aux = []
    for i, (src, dst) in enumerate([(az_h, az), (ay_h, ay), (ry_h, ry), (rz_h, rz), (rx_h, rx), (adv_h, adv), (ax_h, ax)]):
        copy = pltpu.make_async_copy(src, dst, aux_sem.at[i])
        copy.start()
        aux.append(copy)

    barrier = pltpu.get_barrier_semaphore()
    total = 0
    for axis, count, place in zip(AXES, counts, me):
        for k in range(1, count):
            pl.semaphore_signal(barrier, inc=1, device_id={axis: lax.rem(place + k, count)}, device_id_type=MESH)
            total += 1
    for copy in loads:
        copy.wait()

    lane_c = iota((rows, cx), 1)

    def faces_to_rows(load):
        packed = jnp.zeros((rows, cx), f32)
        for v in range(nv):
            moved = pltpu.roll(load(v), 4 * v + 2, 1)
            packed = jnp.where(lane_c // 4 == v, moved, packed)
        return jnp.transpose(packed)[0:pack]

    hx[0] = faces_to_rows(lambda v: uz[v, pl.ds(2 * cy, rows), :])
    pl.semaphore_wait(barrier, total)

    def ring(axis, slot, down_src, down_dst, up_src, up_dst, far_first=False):
        count, place = counts[axis], me[axis]
        lower = lax.rem(place + count - 1, count)
        upper = lax.rem(place + 1, count)
        down = pltpu.make_async_remote_copy(
            src_ref=down_src, dst_ref=down_dst, send_sem=halo_send.at[slot], recv_sem=halo_recv.at[slot],
            device_id={AXES[axis]: lower}, device_id_type=MESH)
        up = pltpu.make_async_remote_copy(
            src_ref=up_src, dst_ref=up_dst, send_sem=halo_send.at[slot + 1], recv_sem=halo_recv.at[slot + 1],
            device_id={AXES[axis]: upper}, device_id_type=MESH)
        if far_first:
            @pl.when(place == count - 1)
            def _():
                up.start()
                down.start()

            @pl.when(place < count - 1)
            def _():
                down.start()
                up.start()
        else:
            down.start()
            up.start()
        return [down, up]

    def spread(axis, src, dst, send, recv):
        count, place = counts[axis], me[axis]
        copies = []
        for k in range(1, count):
            target = lax.rem(place + k, count)
            copy = pltpu.make_async_remote_copy(
                src_ref=src(target), dst_ref=dst, send_sem=send(k - 1), recv_sem=recv(k - 1),
                device_id={AXES[axis]: target}, device_id_type=MESH)
            copy.start()
            copies.append(copy)
        return copies

    z_halo = ring(2, 4,
                  uz.at[:, pl.ds(2 * cy, 2 * cy)], uz.at[:, pl.ds((cz + 2) * cy, 2 * cy)],
                  uz.at[:, pl.ds(cz * cy, 2 * cy)], uz.at[:, pl.ds(0, 2 * cy)], far_first=True)
    x_halo = ring(0, 0, hx.at[0], hx.at[1], hx.at[0], hx.at[2])

    for v in range(nv):
        for y in range(cy):
            uy[v, pl.ds((y + 2) * cz, cz), :] = uz[v, pl.ds(2 * cy + y, cz, stride=cy), :]
    y_halo = ring(1, 2,
                  uy.at[:, pl.ds(2 * cz, 2 * cz)], uy.at[:, pl.ds((cy + 2) * cz, 2 * cz)],
                  uy.at[:, pl.ds(cy * cz, 2 * cz)], uy.at[:, pl.ds(0, 2 * cz)])

    for copy in aux:
        copy.wait()

    every = range(nv)
    octets = cy // 8
    group = kyh.shape[1]
    planes = group // cy
    groups = cz // planes

    def tall(a, times):
        return jnp.broadcast_to(a[:, None, :], (a.shape[0], times, a.shape[1])).reshape(a.shape[0] * times, a.shape[1])

    def again(a, times):
        return jnp.broadcast_to(a[None], (times,) + a.shape).reshape(times * a.shape[0], a.shape[1])

    size_z = kzh.shape[1]
    spread_z = ones_where(iota((cz, size_z), 1) // 8 == iota((cz, size_z), 0))
    spread_y = ones_where(lax.rem(iota((cy, group), 1), cy) == iota((cy, group), 0))
    wide_z = [exact_dot(az[v], spread_z) for v in every]
    wide_y = [exact_dot(ay[v], spread_y) for v in every]
    keep_z = lax.rem(iota((size_z, size_z), 0), 8) == lax.rem(iota((size_z, size_z), 1), 8)
    keep_y = iota((group, group), 0) // cy == iota((group, group), 1) // cy
    for v in every:
        kzh[v], kzl[v] = halves(jnp.where(keep_z, tall(wide_z[v], 8), 0.0))
        kyh[v], kyl[v] = halves(jnp.where(keep_y, again(wide_y[v], planes), 0.0))
        high, low = halves(ax[v])
        axs[v, 0:cx] = jnp.concatenate([high, high], axis=1)
        axs[v, cx:2 * cx] = jnp.concatenate([low, jnp.zeros_like(low)], axis=1)

    nd = wys.shape[1] // cz
    row_y, col_y = iota((nd, 4 * gy), 0), iota((nd, 4 * gy), 1)
    block_y = row_y // nc
    part_y = row_y % nc + (jnp.where(block_y == 0, 2, 0) if nc == 2 else 0)
    pick_y = ones_where((iota((4 * gy, 8), 0) == 4 * me[1] + iota((4 * gy, 8), 1)) & (iota((4 * gy, 8), 1) < 4))
    width_y = wys.shape[2]
    tiled_y = ones_where(lax.rem(iota((8, width_y), 1), 4 * cz) // cz == iota((8, width_y), 0))
    low_y = iota((1, width_y), 1) >= 8 * cz
    same_z = iota((cz, width_y), 0) == lax.rem(iota((cz, width_y), 1), cz)

    def stacked(a, low_lane):
        high = a.astype(bf16).astype(f32)
        return jnp.where(low_lane, a - high, high)

    near_y = [exact_dot(ry[v], pick_y) for v in every]
    given = [exact_dot(coupled(col_y, block_y, part_y, adv[1, v]), near_y[v]) for v in every]
    given = [stacked(exact_dot(given[v], tiled_y), low_y) for v in every]
    mark_y = iota((cy, nc * cx), 1) // cx
    if nc == 2:
        mark_y = jnp.where(me[1] == 0, cy - 2, 0) + mark_y
    else:
        mark_y = jnp.where(mark_y < 2, mark_y, cy - 4 + mark_y)
    mark_y = ones_where(iota((cy, nc * cx), 0) == mark_y)
    for v in every:
        for n in range(nd):
            wys[v, pl.ds(n * cz, cz), :] = jnp.where(same_z, given[v][n:n + 1, :], 0.0).astype(bf16)
        cyt[v] = exact_dot(ay[v], mark_y)

    nz = wts.shape[1] // cy
    row_z, col_z = iota((nz, 4 * gz), 0), iota((nz, 4 * gz), 1)
    dest = row_z // 2
    wanted = jnp.where(dest > me[2], 4 * dest - 2, 4 * dest + 4) + row_z % 2
    sel_z = ones_where((dest != me[2]) & (col_z == wanted) & (dest < gz))
    pick_z = ones_where((iota((4 * gz, 8), 0) == 4 * me[2] + iota((4 * gz, 8), 1)) & (iota((4 * gz, 8), 1) < 4))
    width = wts.shape[2]
    tiled = ones_where(lax.rem(iota((8, width), 1), plane4) // cy == iota((8, width), 0))
    low_lane = iota((1, width), 1) >= 2 * plane4
    same_y = lax.rem(iota((cy, width), 1), cy) == iota((cy, width), 0)

    given = [exact_dot(rz[v], pick_z) for v in every]
    given = [exact_dot(sel_z, given[v]) for v in every]
    given = [stacked(exact_dot(given[v], tiled), low_lane) for v in every]
    for v in every:
        for n in range(nz):
            wts[v, pl.ds(n * cy, cy), :] = jnp.where(same_y, given[v][n:n + 1, :], 0.0).astype(bf16)

    def part(u, direction):
        ahead = fluxes(u[1], direction)
        behind = fluxes(u[-1], direction)
        found = []
        for v in range(nv):
            fourth = u[-2][v] - 4.0 * u[-1][v] + 6.0 * u[0][v] - 4.0 * u[1][v] + u[2][v]
            found.append(-0.5 * (ahead[v] - behind[v]) - damping * fourth)
        return found

    for copy in y_halo:
        copy.wait_recv()

    @pl.loop(0, cy)
    def _(y):
        u = {}
        for off in range(-2, 3):
            at = pl.ds(pl.multiple_of((y + 2 + off) * cz, cz), cz)
            u[off] = [uy[v, at, :] for v in range(nv)]
        found = part(u, 1)
        for v in range(nv):
            res[v, pl.ds(y, cz, stride=cy), :] = found[v]

    for copy in x_halo:
        copy.wait_recv()
    sub4 = iota((4, rows), 0)
    merged = [jnp.where(sub4 < 2, hx[2, 4 * v:4 * v + 4, :], hx[1, 4 * v:4 * v + 4, :]) for v in range(nv)]
    halo_flux = fluxes(merged, 0)
    sub8, lane8 = iota((8, cx), 0), iota((8, cx), 1)

    def at_lane(row, lane, value):
        return jnp.where((sub8 == row) & (lane8 == lane), value, 0.0)

    weights = (at_lane(0, 0, -damping) + at_lane(1, 0, 4.0 * damping) + at_lane(1, 1, -damping)
               + at_lane(2, cx - 2, -damping) + at_lane(2, cx - 1, 4.0 * damping) + at_lane(3, cx - 1, -damping)
               + at_lane(6, cx - 1, -0.5) + at_lane(5, 0, 0.5)).astype(bf16)
    weights = jnp.concatenate([weights, weights], axis=0)
    weights = jnp.concatenate([weights, weights], axis=0)
    for v in range(nv):
        both = jnp.concatenate([merged[v], halo_flux[v]], axis=0)
        high = both.astype(bf16).astype(f32)
        mid = (both - high).astype(bf16).astype(f32)
        parts = jnp.concatenate([high, mid, both - high - mid, jnp.zeros_like(both)], axis=0).astype(bf16)
        edge[v] = one_dot(parts, weights, TN)

    step = cy
    lane = iota((step, cx), 1)

    def shifted(a, offset):
        moved = pltpu.roll(a, (-offset) % cx, 1)
        inside = lane < cx - offset if offset > 0 else lane >= -offset
        return jnp.where(inside, moved, 0.0)

    def body(i, carry):
        squares, top = carry
        base = pl.multiple_of(i * step, step)
        u = {}
        for off in range(-2, 3):
            at = pl.ds(pl.multiple_of(base + (off + 2) * cy, cy), step)
            u[off] = [uz[v, at, :] for v in range(nv)]
        found = part(u, 2)
        values = primitives(u[0])
        velocity, internal, _ = values
        wave = (jnp.abs(velocity[0]) + jnp.abs(velocity[1]) + jnp.abs(velocity[2])
                + jnp.sqrt(3.0 * 1.4 * gas_ratio * internal))
        top = jnp.maximum(top, wave)
        flux_x = fluxes(u[0], 0, values)
        new_squares = []
        for v in range(nv):
            c = u[0][v]
            fourth = (shifted(c, -2) + shifted(c, 2)) - 4.0 * (shifted(c, -1) + shifted(c, 1)) + 6.0 * c
            along_x = -0.5 * (shifted(flux_x[v], 1) - shifted(flux_x[v], -1)) - damping * fourth
            at = pl.ds(base, step)
            value = res[v, at, :] + found[v] + (along_x + edge[v, at, :])
            res[v, at, :] = value
            new_squares.append(squares[v] + value * value)
        return tuple(new_squares), top

    zero = jnp.zeros((step, cx), f32)
    carry = lax.fori_loop(2, cz - 2, body, ((zero,) * nv, zero))
    for copy in z_halo:
        copy.wait_recv()
    squares, top = lax.fori_loop(0, 4, lambda j, c: body(jnp.where(j < 2, j, cz - 4 + j), c), carry)

    y_copies, z_copies = [], []

    def local_x(v):
        both = one_dot(jnp.concatenate(halves(res[v]), axis=1), axs[v], NT)
        res[v] = both[:, 0:cx] + both[:, cx:2 * cx]

    def local_y(v):
        wide = [jnp.concatenate([a[i * group:(i + 1) * group] for i in range(groups)], axis=1) for a in halves(res[v])]
        solved = split_dot((kyh[v], kyl[v]), wide)
        for i in range(groups):
            first[v, pl.ds(i * group, group), :] = solved[:, i * cx:(i + 1) * cx]

    def send_y(v):
        ends = jnp.concatenate(
            [first[v, pl.ds(mark, cz, stride=cy), :] for mark in (0, 1, cy - 2, cy - 1)], axis=0)
        ysend[v] = one_dot(wys[v], stack3(ends))[0:gy * nc * cz].reshape(gy, nc * cz, cx)
        y_copies.append(spread(1, lambda t: ysend.at[v, t], yrecv.at[v, me[1]],
                               lambda k: ys.at[v, k], lambda k: yr.at[v, k]))

    def solve_z(v):
        for copy in y_copies[v]:
            copy.wait_recv()
        taken = ysend[v, me[1]]
        for k in range(1, gy):
            taken = taken + yrecv[v, lax.rem(me[1] + k, gy)]
        value = first[v].reshape(cz, cy, cx)
        for c in range(nc):
            value = value - cyt[v, :, c * cx:(c + 1) * cx][None] * taken[c * cz:(c + 1) * cz][:, None, :]
        wide = jnp.concatenate(
            [value[:, 8 * i:8 * i + 8, :].reshape(size_z, cx) for i in range(octets)], axis=1)
        solved = split_dot((kzh[v], kzl[v]), halves(wide))
        for i in range(octets):
            field[v, :, 8 * i:8 * i + 8, :] = solved[:, i * cx:(i + 1) * cx].reshape(cz, 8, cx)

    def end_planes(v):
        return jnp.concatenate([field[v, 0:2].reshape(2 * cy, cx), field[v, cz - 2:cz].reshape(2 * cy, cx)], axis=0)

    def send_z(v):
        zsend[v] = one_dot(wts[v], stack3(end_planes(v)))[0:gz * 2 * cy].reshape(gz, 2 * cy, cx)
        z_copies.append(spread(2, lambda t: zsend.at[v, t], zrecv.at[v, me[2]],
                               lambda k: zs.at[v, k], lambda k: zr.at[v, k]))

    def in_turn(stages):
        for turn in range(nv + len(stages) - 1):
            for back, stage in enumerate(stages):
                if 0 <= turn - back < nv:
                    stage(turn - back)

    in_turn([local_x, local_y, send_y])

    sub_s = iota((8, cx), 0)
    tile = jnp.where(sub_s == 5, jnp.max(top, axis=0, keepdims=True), 0.0)
    for v in range(nv):
        tile = jnp.where(sub_s == v, jnp.sum(squares[v], axis=0, keepdims=True), tile)
    sty[me[1]] = tile
    stat_copies = [spread(1, lambda t: sty.at[me[1]], sty.at[me[1]], lambda k: ss.at[0, k], lambda k: sr.at[0, k])]

    def gathered(ref, count):
        result = ref[0]
        for q in range(1, count):
            result = jnp.where(sub_s < nv, result + ref[q], jnp.maximum(result, ref[q]))
        return result

    in_turn([solve_z, send_z])

    xb[me[0]] = faces_to_rows(lambda v: field[v].reshape(rows, cx))
    x_copies = [spread(0, lambda t: xb.at[me[0]], xb.at[me[0]], lambda k: xs.at[k], lambda k: xr.at[k])]
    for copy in stat_copies[0]:
        copy.wait_recv()
    stx[me[0]] = gathered(sty, gy)
    stat_copies.append(spread(0, lambda t: stx.at[me[0]], stx.at[me[0]], lambda k: ss.at[1, k], lambda k: sr.at[1, k]))

    mb[...] = jnp.zeros_like(mb)
    cxf[...] = jnp.zeros_like(cxf)
    wide_x = gx * pack
    in_x = lax.rem(iota((4 * gx, wide_x), 1), pack)
    block_x = iota((4 * gx, wide_x), 1) // pack
    row_x = iota((8, 4 * gx), 0)
    placed = [exact_dot(coupled(iota((8, 4 * gx), 1), me[0], row_x, adv[0, v]), rx[v]) for v in every]
    to_pack = [ones_where((in_x // 4 == v) & (iota((4 * gx, wide_x), 0) == 4 * block_x + lax.rem(in_x + 2, 4)))
               for v in every]
    placed = [exact_dot(placed[v], to_pack[v]) for v in every]
    columns = [exact_dot(face_pick((8, cx), cx), ax[v], NT) for v in every]
    for v in every:
        high = columns[v].astype(bf16).astype(f32)
        for k in range(3):
            at = pl.ds(4 * v + 32 * k, 4)
            mb[at, :] = placed[v][0:4]
            cxf[at, v * cx:(v + 1) * cx] = (high if k < 2 else columns[v] - high)[0:4]

    row_l, col_l = iota((8, 4 * gz), 0), iota((8, 4 * gz), 1)
    sel_lf = ones_where((row_l < 4) & (col_l == 4 * me[2] + jnp.where(row_l < 2, row_l - 2, row_l + 2)))
    r8, c8 = iota((8, 8), 0), iota((8, 8), 1)
    near = [exact_dot(sel_lf, rz[v]) for v in every]
    square = [exact_dot(near[v], sel_lf, NT) for v in every]
    own = [exact_dot(near[v], pick_z) for v in every]
    columns = [exact_dot(az[v], face_pick((8, cz), cz), NT) for v in every]

    def mixed(v):
        def e(i, j):
            return square[v][i:i + 1, j:j + 1]

        det_l = e(0, 0) * e(1, 1) - e(0, 1) * e(1, 0)
        det_f = e(2, 2) * e(3, 3) - e(2, 3) * e(3, 2)
        inv_l = 1.0 / jnp.where(me[2] > 0, det_l, 1.0)
        inv_f = 1.0 / jnp.where(me[2] < gz - 1, det_f, 1.0)
        mix = ones_where((r8 == c8) & (r8 < 4))
        for i in range(2):
            for j, value in enumerate([(e(2 + i, 0) * e(1, 1) - e(2 + i, 1) * e(1, 0)) * inv_l,
                                       (e(2 + i, 1) * e(0, 0) - e(2 + i, 0) * e(0, 1)) * inv_l]):
                mix = jnp.where((r8 == 2 + i) & (c8 == j), value, mix)
            for j, value in enumerate([(e(i, 2) * e(3, 3) - e(i, 3) * e(3, 2)) * inv_f,
                                       (e(i, 3) * e(2, 2) - e(i, 2) * e(2, 3)) * inv_f]):
                mix = jnp.where((r8 == i) & (c8 == 2 + j), value, mix)
        return mix

    def weighed(v):
        speed = adv[2, v]
        weigh = jnp.where((r8 == c8) & (r8 < 4), fourth_coef, 0.0)
        weigh = jnp.where((r8 == 0) & (c8 == 1), -0.5 * speed - 4.0 * fourth_coef, weigh)
        return jnp.where((r8 == 3) & (c8 == 2), 0.5 * speed - 4.0 * fourth_coef, weigh).astype(f32)

    own = [exact_dot(weighed(v), own[v]) for v in every]
    peers = [exact_dot(weighed(v), mixed(v)) for v in every]
    own = [exact_dot(own[v], tiled) for v in every]
    peers = [exact_dot(peers[v], tiled) for v in every]
    own = [stacked(exact_dot(columns[v], own[v]), low_lane) for v in every]
    peers = [stacked(exact_dot(columns[v], peers[v]), low_lane) for v in every]
    for v in every:
        for z in range(cz):
            pto[v, pl.ds(z * cy, cy), :] = jnp.where(same_y, own[v][z:z + 1, :], 0.0).astype(bf16)
            pts[v, pl.ds(z * cy, cy), :] = jnp.where(same_y, peers[v][z:z + 1, :], 0.0).astype(bf16)

    for v in every:
        field[v] = field[v] - one_dot(pto[v], stack3(end_planes(v))).reshape(cz, cy, cx)

    for group in x_copies + [stat_copies[1]]:
        for copy in group:
            copy.wait_recv()
    stz[me[2]] = gathered(stx, gx)
    stat_copies.append(spread(2, lambda t: stz.at[me[2]], stz.at[me[2]], lambda k: ss.at[2, k], lambda k: sr.at[2, k]))

    ext[...] = jnp.transpose(split_dot(halves(mb[...]), halves(xb[...].reshape(wide_x, rows))))
    lane_e = iota((plane4, cx), 1)
    lane_v = jnp.where(lane_e < 96, (lane_e % 32) // 4, -1)
    ends = jnp.concatenate([ext[pl.ds(0, 2 * cy), :], ext[pl.ds((cz - 2) * cy, 2 * cy), :]], axis=0)

    def by_variable(table, a):
        result = None
        for v in range(nv):
            term = one_dot(table[v], stack3(jnp.where(lane_v == v, a, 0.0)))
            result = term if result is None else result + term
        return result

    esend[...] = by_variable(wts, ends)[0:gz * 2 * cy].reshape(gz, 2 * cy, cx)
    e_copies = spread(2, lambda t: esend.at[t], erecv.at[me[2]], lambda k: es.at[k], lambda k: er.at[k])
    ext[...] = ext[...] - by_variable(pto, ends)

    def sides(load):
        before, after = None, None
        for k in range(1, gz):
            q = lax.rem(me[2] + k, gz)
            value = load(q)
            left, right = jnp.where(q < me[2], value, 0.0), jnp.where(q > me[2], value, 0.0)
            before = left if before is None else before + left
            after = right if after is None else after + right
        return jnp.concatenate([before, after], axis=0)

    for v in range(nv):
        for copy in z_copies[v]:
            copy.wait_recv()
        field[v] = field[v] - one_dot(pts[v], stack3(sides(lambda q: zrecv[v, q]))).reshape(cz, cy, cx)

    for copy in stat_copies[2]:
        copy.wait_recv()
    final = gathered(stz, gz)
    norm = jnp.sqrt(jnp.sum(final, axis=1, keepdims=True) / float(cells))
    fastest = courant / jnp.max(final, axis=1, keepdims=True)
    stats_out[...] = jnp.broadcast_to(norm, (8, cx))
    time_step = fastest[5:6, :]

    for copy in e_copies:
        copy.wait_recv()
    solved = ext[...] - by_variable(pts, sides(lambda q: erecv[q]))
    high = solved.astype(bf16).astype(f32)
    parts = jnp.where((lane_c >= 32) & (lane_c < 64), solved - high, high).astype(bf16)
    for v in range(nv):
        out[v] = (field[v].reshape(rows, cx) - one_dot(parts, cxf[:, v * cx:(v + 1) * cx].astype(bf16))) * time_step

    for group in [x_halo, y_halo, z_halo, e_copies] + x_copies + y_copies + z_copies + stat_copies:
        for copy in group:
            copy.wait_send()


def finish(nv, solved, stats, update, norm, sem):
    copies = []
    for v in range(nv):
        copy = pltpu.make_async_copy(solved.at[v], update.at[v], sem.at[v])
        copy.start()
        copies.append(copy)
    for v in range(nv):
        norm[v] = stats[v, 0]
    for copy in copies:
        copy.wait()


def shards(counts, flow_state, advection, inverse_x, inverse_y, inverse_z, reduced_x, reduced_y, reduced_z):
    nv, cz, cy, cx = flow_state.shape
    gx, gy, gz = counts
    rows = cz * cy
    cells = rows * cx * gx * gy * gz
    most = max(counts) - 1
    hbm = pl.BlockSpec(memory_space=pltpu.HBM)
    vmem = pl.BlockSpec(memory_space=pltpu.VMEM)
    dma = pltpu.SemaphoreType.DMA
    pack = -(-4 * nv // 8) * 8
    nc = 2 if gy == 2 else 4
    nd = max(8, gy * nc)
    nz = max(8, 2 * gz)
    width = 12 * cy
    group = cy * min(cz, max(1, 256 // cy))
    out, stats = pl.pallas_call(
        functools.partial(kernel, (counts, nv, cz, cy, cx, cells)),
        out_shape=(pltpu.VMEM((nv, rows, cx), f32), pltpu.VMEM((8, cx), f32)),
        in_specs=[hbm] * 8,
        out_specs=(vmem, vmem),
        scratch_shapes=[
            pltpu.VMEM((nv, (cz + 4) * cy, cx), f32),
            pltpu.VMEM((nv, (cy + 4) * cz, cx), f32),
            pltpu.VMEM((3, pack, rows), f32),
            pltpu.VMEM((nv, rows, cx), f32),
            pltpu.VMEM((nv, rows, cx), f32),
            pltpu.VMEM((nv, cz, cy, cx), f32),
            pltpu.VMEM((nv, rows, cx), f32),
            pltpu.VMEM((rows, cx), f32),
            pltpu.VMEM((nv, nd * cz, 12 * cz), bf16),
            pltpu.VMEM((nv, nz * cy, width), bf16),
            pltpu.VMEM((nv, rows, width), bf16),
            pltpu.VMEM((nv, rows, width), bf16),
            pltpu.VMEM((nv, 8 * cz, 8 * cz), bf16),
            pltpu.VMEM((nv, 8 * cz, 8 * cz), bf16),
            pltpu.VMEM((nv, group, group), bf16),
            pltpu.VMEM((nv, group, group), bf16),
            pltpu.VMEM((nv, 2 * cx, 2 * cx), bf16),
            pltpu.VMEM((nv, cy, nc * cx), f32),
            pltpu.VMEM((cx, gx * pack), f32),
            pltpu.VMEM((cx, nv * cx), f32),
            pltpu.VMEM((gx, pack, rows), f32),
            pltpu.VMEM((nv, gy, nc * cz, cx), f32),
            pltpu.VMEM((nv, gy, nc * cz, cx), f32),
            pltpu.VMEM((nv, gz, 2 * cy, cx), f32),
            pltpu.VMEM((nv, gz, 2 * cy, cx), f32),
            pltpu.VMEM((gz, 2 * cy, cx), f32),
            pltpu.VMEM((gz, 2 * cy, cx), f32),
            pltpu.VMEM((gx, 8, cx), f32),
            pltpu.VMEM((gy, 8, cx), f32),
            pltpu.VMEM((gz, 8, cx), f32),
            pltpu.VMEM(inverse_x.shape, f32),
            pltpu.VMEM(inverse_y.shape, f32),
            pltpu.VMEM(inverse_z.shape, f32),
            pltpu.VMEM(reduced_x.shape, f32),
            pltpu.VMEM(reduced_y.shape, f32),
            pltpu.VMEM(reduced_z.shape, f32),
            pltpu.SMEM(advection.shape, f32),
            dma((nv,)),
            dma((7,)),
            dma((6,)), dma((6,)),
            dma((gx - 1,)), dma((gx - 1,)),
            dma((nv, gy - 1)), dma((nv, gy - 1)),
            dma((nv, gz - 1)), dma((nv, gz - 1)),
            dma((gz - 1,)), dma((gz - 1,)),
            dma((3, most)), dma((3, most)),
        ],
        compiler_params=pltpu.CompilerParams(
            collective_id=0, has_side_effects=True, vmem_limit_bytes=60 * 1024 * 1024),
    )(flow_state.reshape(nv, rows, cx), advection, inverse_x, inverse_y, inverse_z, reduced_x, reduced_y, reduced_z)
    update, norm = pl.pallas_call(
        functools.partial(finish, nv),
        out_shape=(jax.ShapeDtypeStruct((nv, rows, cx), f32), jax.ShapeDtypeStruct((nv,), f32)),
        in_specs=[vmem, vmem],
        out_specs=(pl.BlockSpec(memory_space=pltpu.HBM), pl.BlockSpec(memory_space=pltpu.SMEM)),
        scratch_shapes=[dma((nv,))],
        compiler_params=pltpu.CompilerParams(vmem_limit_bytes=4 * 1024 * 1024),
    )(out, stats)
    return update.reshape(flow_state.shape), norm


def solution(mesh):
    counts = tuple(mesh.shape[axis] for axis in AXES)
    placed = (P(None, "gz", "gy", "gx"), P(), P(), P(), P(), P(), P(), P())
    return jax.shard_map(
        functools.partial(shards, counts),
        mesh=mesh,
        in_specs=placed,
        out_specs=(P(None, "gz", "gy", "gx"), P()),
        check_vma=False,
    )
```

```python
import functools

import jax
import jax.numpy as jnp
from jax import lax
from jax.experimental import pallas as pl
from jax.experimental.pallas import tpu as pltpu
from jax.sharding import PartitionSpec as P

MESH = pl.DeviceIdType.MESH
HIGHEST = lax.Precision.HIGHEST
gas_ratio = 0.4
courant = 8000.0
damping = 0.0625
fourth_coef = 0.5
AXES = ("gx", "gy", "gz")
f32 = jnp.float32
bf16 = jnp.bfloat16

NN = (((1,), (0,)), ((), ()))
NT = (((1,), (1,)), ((), ()))
TN = (((0,), (0,)), ((), ()))


def exact_dot(a, b, dims=NN):
    return lax.dot_general(a, b, dims, precision=HIGHEST, preferred_element_type=f32)


def one_dot(a, b, dims=NN):
    return lax.dot_general(a, b, dims, preferred_element_type=f32)


def halves(a):
    high = a.astype(bf16)
    low = (a - high.astype(f32)).astype(bf16)
    return high, low


def split_dot(a, b, dims=NN):
    return one_dot(a[0], b[0], dims) + (one_dot(a[0], b[1], dims) + one_dot(a[1], b[0], dims))


def stack3(a):
    high, low = halves(a)
    return jnp.concatenate([high, low, high], axis=0)


def iota(shape, dim):
    return lax.broadcasted_iota(jnp.int32, shape, dim)


def ones_where(mask):
    return jnp.where(mask, 1.0, 0.0).astype(f32)


def primitives(u):
    inverse = 1.0 / u[0]
    velocity = [u[1] * inverse, u[2] * inverse, u[3] * inverse]
    kinetic = 0.5 * (velocity[0] * velocity[0] + velocity[1] * velocity[1] + velocity[2] * velocity[2])
    internal = jnp.maximum(u[4] * inverse - kinetic, 0.25)
    pressure = gas_ratio * u[0] * internal
    return velocity, internal, pressure


def fluxes(u, direction, values=None):
    velocity, internal, pressure = primitives(u) if values is None else values
    carried = velocity[direction]
    found = [u[1 + direction]]
    for component in range(3):
        moment = u[1 + component] * carried
        if component == direction:
            moment = moment + pressure
        found.append(moment)
    found.append((u[4] + pressure) * carried)
    return found


def coupled(col, block, part, speed):
    lower = -0.5 * speed - 4.0 * fourth_coef
    upper = 0.5 * speed - 4.0 * fourth_coef
    value = jnp.where((part == 0) & (col == 4 * block - 2), fourth_coef, 0.0)
    value = jnp.where((part == 0) & (col == 4 * block - 1), lower, value)
    value = jnp.where((part == 1) & (col == 4 * block - 1), fourth_coef, value)
    value = jnp.where((part == 2) & (col == 4 * block + 4), fourth_coef, value)
    value = jnp.where((part == 3) & (col == 4 * block + 4), upper, value)
    return jnp.where((part == 3) & (col == 4 * block + 5), fourth_coef, value).astype(f32)


def face_pick(shape, size, row_dim=0):
    r, c = iota(shape, row_dim), iota(shape, 1 - row_dim)
    return ones_where((r < 4) & (c == jnp.where(r < 2, r, size - 4 + r)))


def kernel(dims, state_h, adv_h, ax_h, ay_h, az_h, rx_h, ry_h, rz_h, out, stats_out,
           uz, uy, vel, prs, hx, res, edge, field, first, ext, wys, wts, pts, pto, kzh, kzl, kyh, kyl, axs, cyt, mb, cxf, cxb,
           xb, ysend, yrecv, zsend, zrecv, esend, erecv, stx, sty, stz,
           ax, ay, az, rx, ry, rz, adv,
           in_sem, aux_sem, halo_send, halo_recv, xs, xr, ys, yr, zs, zr, es, er, ss, sr):
    counts, nv, cz, cy, cx, cells = dims
    gx, gy, gz = counts
    rows = cz * cy
    pack = xb.shape[1]
    nc = 2 if gy == 2 else 4
    plane4 = 4 * cy
    me = [lax.axis_index(axis) for axis in AXES]

    loads = []
    for v in range(nv):
        copy = pltpu.make_async_copy(state_h.at[v], uz.at[v, pl.ds(2 * cy, rows)], in_sem.at[v])
        copy.start()
        loads.append(copy)
    aux = []
    for i, (src, dst) in enumerate([(az_h, az), (ay_h, ay), (ry_h, ry), (rz_h, rz), (rx_h, rx), (adv_h, adv), (ax_h, ax)]):
        copy = pltpu.make_async_copy(src, dst, aux_sem.at[i])
        copy.start()
        aux.append(copy)

    barrier = pltpu.get_barrier_semaphore()
    total = 0
    for axis, count, place in zip(AXES, counts, me):
        for k in range(1, count):
            pl.semaphore_signal(barrier, inc=1, device_id={axis: lax.rem(place + k, count)}, device_id_type=MESH)
            total += 1
    for copy in loads:
        copy.wait()

    lane_c = iota((rows, cx), 1)

    def faces_to_rows(load):
        packed = jnp.zeros((rows, cx), f32)
        for v in range(nv):
            moved = pltpu.roll(load(v), 4 * v + 2, 1)
            packed = jnp.where(lane_c // 4 == v, moved, packed)
        return jnp.transpose(packed)[0:pack]

    pl.semaphore_wait(barrier, total)

    def ring(axis, slot, down_src, down_dst, up_src, up_dst, far_first=False):
        count, place = counts[axis], me[axis]
        lower = lax.rem(place + count - 1, count)
        upper = lax.rem(place + 1, count)
        down = pltpu.make_async_remote_copy(
            src_ref=down_src, dst_ref=down_dst, send_sem=halo_send.at[slot], recv_sem=halo_recv.at[slot],
            device_id={AXES[axis]: lower}, device_id_type=MESH)
        up = pltpu.make_async_remote_copy(
            src_ref=up_src, dst_ref=up_dst, send_sem=halo_send.at[slot + 1], recv_sem=halo_recv.at[slot + 1],
            device_id={AXES[axis]: upper}, device_id_type=MESH)
        if far_first:
            @pl.when(place == count - 1)
            def _():
                up.start()
                down.start()

            @pl.when(place < count - 1)
            def _():
                down.start()
                up.start()
        else:
            down.start()
            up.start()
        return [down, up]

    def spread(axis, src, dst, send, recv):
        count, place = counts[axis], me[axis]
        copies = []
        for k in range(1, count):
            target = lax.rem(place + k, count)
            copy = pltpu.make_async_remote_copy(
                src_ref=src(target), dst_ref=dst, send_sem=send(k - 1), recv_sem=recv(k - 1),
                device_id={AXES[axis]: target}, device_id_type=MESH)
            copy.start()
            copies.append(copy)
        return copies

    z_halo = ring(2, 4,
                  uz.at[:, pl.ds(2 * cy, 2 * cy)], uz.at[:, pl.ds((cz + 2) * cy, 2 * cy)],
                  uz.at[:, pl.ds(cz * cy, 2 * cy)], uz.at[:, pl.ds(0, 2 * cy)], far_first=True)
    hx[0] = faces_to_rows(lambda v: uz[v, pl.ds(2 * cy, rows), :])

    x_halo = ring(0, 0, hx.at[0], hx.at[1], hx.at[0], hx.at[2])

    for v in range(nv):
        for y in range(cy):
            uy[v, pl.ds((y + 2) * cz, cz), :] = uz[v, pl.ds(2 * cy + y, cz, stride=cy), :]
    y_halo = ring(1, 2,
                  uy.at[:, pl.ds(2 * cz, 2 * cz)], uy.at[:, pl.ds((cy + 2) * cz, 2 * cz)],
                  uy.at[:, pl.ds(cy * cz, 2 * cz)], uy.at[:, pl.ds(0, 2 * cz)])

    def derive(start, size):
        at = pl.ds(start, size)
        velocity, internal, pressure = primitives([uz[v, at, :] for v in range(nv)])
        for j in range(3):
            vel[j, at, :] = velocity[j]
        prs[at, :] = pressure
        return (jnp.abs(velocity[0]) + jnp.abs(velocity[1]) + jnp.abs(velocity[2])
                + jnp.sqrt(3.0 * 1.4 * gas_ratio * internal))

    chunk = 4 * cy
    top = lax.fori_loop(
        0, rows // chunk,
        lambda i, top: jnp.maximum(top, derive(pl.multiple_of(2 * cy + i * chunk, 8), chunk)),
        jnp.zeros((chunk, cx), f32))

    for copy in aux:
        copy.wait()

    every = range(nv)
    octets = cy // 8
    group = kyh.shape[1]
    planes = group // cy
    groups = cz // planes

    def tall(a, times):
        return jnp.broadcast_to(a[:, None, :], (a.shape[0], times, a.shape[1])).reshape(a.shape[0] * times, a.shape[1])

    def again(a, times):
        return jnp.broadcast_to(a[None], (times,) + a.shape).reshape(times * a.shape[0], a.shape[1])

    size_z = kzh.shape[1]
    spread_z = ones_where(iota((cz, size_z), 1) // 8 == iota((cz, size_z), 0))
    spread_y = ones_where(lax.rem(iota((cy, group), 1), cy) == iota((cy, group), 0))
    wide_z = [exact_dot(az[v], spread_z) for v in every]
    wide_y = [exact_dot(ay[v], spread_y) for v in every]
    keep_z = lax.rem(iota((size_z, size_z), 0), 8) == lax.rem(iota((size_z, size_z), 1), 8)
    keep_y = iota((group, group), 0) // cy == iota((group, group), 1) // cy
    for v in every:
        kzh[v], kzl[v] = halves(jnp.where(keep_z, tall(wide_z[v], 8), 0.0))
        kyh[v], kyl[v] = halves(jnp.where(keep_y, again(wide_y[v], planes), 0.0))
        high, low = halves(ax[v])
        axs[v, 0:cx] = jnp.concatenate([high, high], axis=1)
        axs[v, cx:2 * cx] = jnp.concatenate([low, jnp.zeros_like(low)], axis=1)

    nd = wys.shape[1] // cz
    row_y, col_y = iota((nd, 4 * gy), 0), iota((nd, 4 * gy), 1)
    block_y = row_y // nc
    part_y = row_y % nc + (jnp.where(block_y == 0, 2, 0) if nc == 2 else 0)
    pick_y = ones_where((iota((4 * gy, 8), 0) == 4 * me[1] + iota((4 * gy, 8), 1)) & (iota((4 * gy, 8), 1) < 4))
    width_y = wys.shape[2]
    tiled_y = ones_where(lax.rem(iota((8, width_y), 1), 4 * cz) // cz == iota((8, width_y), 0))
    low_y = iota((1, width_y), 1) >= 8 * cz
    same_z = iota((cz, width_y), 0) == lax.rem(iota((cz, width_y), 1), cz)

    def stacked(a, low_lane):
        high = a.astype(bf16).astype(f32)
        return jnp.where(low_lane, a - high, high)

    near_y = [exact_dot(ry[v], pick_y) for v in every]
    given = [exact_dot(coupled(col_y, block_y, part_y, adv[1, v]), near_y[v]) for v in every]
    given = [stacked(exact_dot(given[v], tiled_y), low_y) for v in every]
    mark_y = iota((cy, nc * cx), 1) // cx
    if nc == 2:
        mark_y = jnp.where(me[1] == 0, cy - 2, 0) + mark_y
    else:
        mark_y = jnp.where(mark_y < 2, mark_y, cy - 4 + mark_y)
    mark_y = ones_where(iota((cy, nc * cx), 0) == mark_y)
    for v in every:
        for n in range(nd):
            wys[v, pl.ds(n * cz, cz), :] = jnp.where(same_z, given[v][n:n + 1, :], 0.0).astype(bf16)
        cyt[v] = exact_dot(ay[v], mark_y)

    nz = wts.shape[1] // cy
    row_z, col_z = iota((nz, 4 * gz), 0), iota((nz, 4 * gz), 1)
    dest = row_z // 2
    wanted = jnp.where(dest > me[2], 4 * dest - 2, 4 * dest + 4) + row_z % 2
    sel_z = ones_where((dest != me[2]) & (col_z == wanted) & (dest < gz))
    pick_z = ones_where((iota((4 * gz, 8), 0) == 4 * me[2] + iota((4 * gz, 8), 1)) & (iota((4 * gz, 8), 1) < 4))
    width = wts.shape[2]
    tiled = ones_where(lax.rem(iota((8, width), 1), plane4) // cy == iota((8, width), 0))
    low_lane = iota((1, width), 1) >= 2 * plane4
    same_y = lax.rem(iota((cy, width), 1), cy) == iota((cy, width), 0)

    given = [exact_dot(rz[v], pick_z) for v in every]
    given = [exact_dot(sel_z, given[v]) for v in every]
    given = [stacked(exact_dot(given[v], tiled), low_lane) for v in every]
    for v in every:
        for n in range(nz):
            wts[v, pl.ds(n * cy, cy), :] = jnp.where(same_y, given[v][n:n + 1, :], 0.0).astype(bf16)

    def part(u, direction):
        ahead = fluxes(u[1], direction)
        behind = fluxes(u[-1], direction)
        found = []
        for v in range(nv):
            fourth = u[-2][v] - 4.0 * u[-1][v] + 6.0 * u[0][v] - 4.0 * u[1][v] + u[2][v]
            found.append(-0.5 * (ahead[v] - behind[v]) - damping * fourth)
        return found

    for copy in y_halo:
        copy.wait_recv()

    @pl.loop(0, cy)
    def _(y):
        u = {}
        for off in range(-2, 3):
            at = pl.ds(pl.multiple_of((y + 2 + off) * cz, cz), cz)
            u[off] = [uy[v, at, :] for v in range(nv)]
        found = part(u, 1)
        for v in range(nv):
            res[v, pl.ds(y, cz, stride=cy), :] = found[v]

    for copy in x_halo:
        copy.wait_recv()
    sub4 = iota((4, rows), 0)
    merged = [jnp.where(sub4 < 2, hx[2, 4 * v:4 * v + 4, :], hx[1, 4 * v:4 * v + 4, :]) for v in range(nv)]
    nearest = [hx[0, 4 * v:4 * v + 4, :] for v in range(nv)]
    halo_flux = [a - b for a, b in zip(fluxes(merged, 0), fluxes(nearest, 0))]
    merged = [a - b for a, b in zip(merged, nearest)]
    sub8, lane8 = iota((8, cx), 0), iota((8, cx), 1)

    def at_lane(row, lane, value):
        return jnp.where((sub8 == row) & (lane8 == lane), value, 0.0)

    weights = (at_lane(0, 0, -damping) + at_lane(1, 0, 4.0 * damping) + at_lane(1, 1, -damping)
               + at_lane(2, cx - 2, -damping) + at_lane(2, cx - 1, 4.0 * damping) + at_lane(3, cx - 1, -damping)
               + at_lane(6, cx - 1, -0.5) + at_lane(5, 0, 0.5)).astype(bf16)
    weights = jnp.concatenate([weights, weights], axis=0)
    weights = jnp.concatenate([weights, weights], axis=0)
    for v in range(nv):
        both = jnp.concatenate([merged[v], halo_flux[v]], axis=0)
        high = both.astype(bf16).astype(f32)
        mid = (both - high).astype(bf16).astype(f32)
        parts = jnp.concatenate([high, mid, both - high - mid, jnp.zeros_like(both)], axis=0).astype(bf16)
        edge[v] = one_dot(parts, weights, TN)

    def residual(base, planes, squares):
        size = planes * cy
        here = pl.ds(base + 2 * cy, size)
        vx, pc = vel[0, here, :], prs[here, :]
        around = pl.ds(base + cy, size + 2 * cy)
        vz, pz = vel[2, around, :], prs[around, :]
        found = []
        for v in range(nv):
            u = uz[v, pl.ds(base, size + 4 * cy), :]
            inner = u[cy:size + 3 * cy]
            c = u[2 * cy:size + 2 * cy]
            if v == 0:
                flux_x, flux_z = uz[1, here, :], uz[3, around, :]
            elif v == 4:
                flux_x, flux_z = (c + pc) * vx, (inner + pz) * vz
            else:
                flux_x = c * vx + pc if v == 1 else c * vx
                flux_z = inner * vz + pz if v == 3 else inner * vz
            beside = inner[0:size] + inner[2 * cy:size + 2 * cy]
            beyond = u[0:size] + u[4 * cy:size + 4 * cy]
            along_z = 0.5 * (flux_z[0:size] - flux_z[2 * cy:size + 2 * cy]) + (4.0 * damping * beside - damping * beyond)
            near, half, far = 4.0 * damping * c, 0.5 * flux_x, -damping * c
            along_x = ((pltpu.roll(near - half, cx - 1, 1) + pltpu.roll(near + half, 1, 1))
                       + (pltpu.roll(far, cx - 2, 1) + pltpu.roll(far, 2, 1)))
            at = pl.ds(base, size)
            value = (res[v, at, :] + edge[v, at, :]) + (along_z + along_x) - 12.0 * damping * c
            res[v, at, :] = value
            found.append(squares[v] + jnp.sum((value * value).reshape(planes, cy, cx), axis=0))
        return tuple(found)

    planes_in = next(n for n in (7, 4, 2, 1) if (cz - 4) % n == 0)
    squares = lax.fori_loop(
        0, (cz - 4) // planes_in,
        lambda i, c: residual(pl.multiple_of(2 * cy + i * planes_in * cy, 8), planes_in, c),
        (jnp.zeros((cy, cx), f32),) * nv)
    for copy in z_halo:
        copy.wait_recv()
    derive(0, 2 * cy)
    derive((cz + 2) * cy, 2 * cy)
    squares = residual(0, 2, squares)
    squares = residual((cz - 2) * cy, 2, squares)

    sub_s = iota((8, cx), 0)
    tile = jnp.where(sub_s == 5, jnp.max(top, axis=0, keepdims=True), 0.0)
    for v in range(nv):
        tile = jnp.where(sub_s == v, jnp.sum(squares[v], axis=0, keepdims=True), tile)
    sty[me[1]] = tile
    stat_copies = [spread(1, lambda t: sty.at[me[1]], sty.at[me[1]], lambda k: ss.at[0, k], lambda k: sr.at[0, k])]

    y_copies, z_copies = [], []

    def local_x(v):
        both = one_dot(jnp.concatenate(halves(res[v]), axis=1), axs[v], NT)
        res[v] = both[:, 0:cx] + both[:, cx:2 * cx]

    def local_y(v):
        wide = [jnp.concatenate([a[i * group:(i + 1) * group] for i in range(groups)], axis=1) for a in halves(res[v])]
        solved = split_dot((kyh[v], kyl[v]), wide)
        for i in range(groups):
            first[v, pl.ds(i * group, group), :] = solved[:, i * cx:(i + 1) * cx]

    def send_y(v):
        ends = jnp.concatenate(
            [first[v, pl.ds(mark, cz, stride=cy), :] for mark in (0, 1, cy - 2, cy - 1)], axis=0)
        ysend[v] = one_dot(wys[v], stack3(ends))[0:gy * nc * cz].reshape(gy, nc * cz, cx)
        y_copies.append(spread(1, lambda t: ysend.at[v, t], yrecv.at[v, me[1]],
                               lambda k: ys.at[v, k], lambda k: yr.at[v, k]))

    def solve_z(v):
        for copy in y_copies[v]:
            copy.wait_recv()
        taken = ysend[v, me[1]]
        for k in range(1, gy):
            taken = taken + yrecv[v, lax.rem(me[1] + k, gy)]
        value = first[v].reshape(cz, cy, cx)
        for c in range(nc):
            value = value - cyt[v, :, c * cx:(c + 1) * cx][None] * taken[c * cz:(c + 1) * cz][:, None, :]
        wide = jnp.concatenate(
            [value[:, 8 * i:8 * i + 8, :].reshape(size_z, cx) for i in range(octets)], axis=1)
        solved = split_dot((kzh[v], kzl[v]), halves(wide))
        for i in range(octets):
            field[v, :, 8 * i:8 * i + 8, :] = solved[:, i * cx:(i + 1) * cx].reshape(cz, 8, cx)

    def end_planes(v):
        return jnp.concatenate([field[v, 0:2].reshape(2 * cy, cx), field[v, cz - 2:cz].reshape(2 * cy, cx)], axis=0)

    def send_z(v):
        zsend[v] = one_dot(wts[v], stack3(end_planes(v)))[0:gz * 2 * cy].reshape(gz, 2 * cy, cx)
        z_copies.append(spread(2, lambda t: zsend.at[v, t], zrecv.at[v, me[2]],
                               lambda k: zs.at[v, k], lambda k: zr.at[v, k]))

    def gathered(ref, count):
        result = ref[0]
        for q in range(1, count):
            result = jnp.where(sub_s < nv, result + ref[q], jnp.maximum(result, ref[q]))
        return result

    for turn in range(nv + 2):
        if turn < nv:
            local_x(turn)
        if turn >= 2:
            solve_z(turn - 2)
        if turn < nv:
            local_y(turn)
        if turn >= 2:
            send_z(turn - 2)
        if turn < nv:
            send_y(turn)

    xb[me[0]] = faces_to_rows(lambda v: field[v].reshape(rows, cx))
    x_copies = [spread(0, lambda t: xb.at[me[0]], xb.at[me[0]], lambda k: xs.at[k], lambda k: xr.at[k])]
    for copy in stat_copies[0]:
        copy.wait_recv()
    stx[me[0]] = gathered(sty, gy)
    stat_copies.append(spread(0, lambda t: stx.at[me[0]], stx.at[me[0]], lambda k: ss.at[1, k], lambda k: sr.at[1, k]))

    mb[...] = jnp.zeros_like(mb)
    cxf[...] = jnp.zeros_like(cxf)
    wide_x = gx * pack
    in_x = lax.rem(iota((4 * gx, wide_x), 1), pack)
    block_x = iota((4 * gx, wide_x), 1) // pack
    row_x = iota((8, 4 * gx), 0)
    placed = [exact_dot(coupled(iota((8, 4 * gx), 1), me[0], row_x, adv[0, v]), rx[v]) for v in every]
    to_pack = [ones_where((in_x // 4 == v) & (iota((4 * gx, wide_x), 0) == 4 * block_x + lax.rem(in_x + 2, 4)))
               for v in every]
    placed = [exact_dot(placed[v], to_pack[v]) for v in every]
    columns = [exact_dot(face_pick((8, cx), cx), ax[v], NT) for v in every]
    for v in every:
        high = columns[v].astype(bf16).astype(f32)
        for k in range(3):
            at = pl.ds(4 * v + 32 * k, 4)
            mb[at, :] = placed[v][0:4]
            cxf[at, v * cx:(v + 1) * cx] = (high if k < 2 else columns[v] - high)[0:4]

    cxb[...] = cxf[...].astype(bf16)

    row_l, col_l = iota((8, 4 * gz), 0), iota((8, 4 * gz), 1)
    sel_lf = ones_where((row_l < 4) & (col_l == 4 * me[2] + jnp.where(row_l < 2, row_l - 2, row_l + 2)))
    r8, c8 = iota((8, 8), 0), iota((8, 8), 1)
    near = [exact_dot(sel_lf, rz[v]) for v in every]
    square = [exact_dot(near[v], sel_lf, NT) for v in every]
    own = [exact_dot(near[v], pick_z) for v in every]
    columns = [exact_dot(az[v], face_pick((8, cz), cz), NT) for v in every]

    def mixed(v):
        def e(i, j):
            return square[v][i:i + 1, j:j + 1]

        det_l = e(0, 0) * e(1, 1) - e(0, 1) * e(1, 0)
        det_f = e(2, 2) * e(3, 3) - e(2, 3) * e(3, 2)
        inv_l = 1.0 / jnp.where(me[2] > 0, det_l, 1.0)
        inv_f = 1.0 / jnp.where(me[2] < gz - 1, det_f, 1.0)
        mix = ones_where((r8 == c8) & (r8 < 4))
        for i in range(2):
            for j, value in enumerate([(e(2 + i, 0) * e(1, 1) - e(2 + i, 1) * e(1, 0)) * inv_l,
                                       (e(2 + i, 1) * e(0, 0) - e(2 + i, 0) * e(0, 1)) * inv_l]):
                mix = jnp.where((r8 == 2 + i) & (c8 == j), value, mix)
            for j, value in enumerate([(e(i, 2) * e(3, 3) - e(i, 3) * e(3, 2)) * inv_f,
                                       (e(i, 3) * e(2, 2) - e(i, 2) * e(2, 3)) * inv_f]):
                mix = jnp.where((r8 == i) & (c8 == 2 + j), value, mix)
        return mix

    def weighed(v):
        speed = adv[2, v]
        weigh = jnp.where((r8 == c8) & (r8 < 4), fourth_coef, 0.0)
        weigh = jnp.where((r8 == 0) & (c8 == 1), -0.5 * speed - 4.0 * fourth_coef, weigh)
        return jnp.where((r8 == 3) & (c8 == 2), 0.5 * speed - 4.0 * fourth_coef, weigh).astype(f32)

    own = [exact_dot(weighed(v), own[v]) for v in every]
    peers = [exact_dot(weighed(v), mixed(v)) for v in every]
    own = [exact_dot(own[v], tiled) for v in every]
    peers = [exact_dot(peers[v], tiled) for v in every]
    own = [stacked(exact_dot(columns[v], own[v]), low_lane) for v in every]
    peers = [stacked(exact_dot(columns[v], peers[v]), low_lane) for v in every]
    for v in every:
        for z in range(cz):
            pto[v, pl.ds(z * cy, cy), :] = jnp.where(same_y, own[v][z:z + 1, :], 0.0).astype(bf16)
            pts[v, pl.ds(z * cy, cy), :] = jnp.where(same_y, peers[v][z:z + 1, :], 0.0).astype(bf16)

    for v in every:
        field[v] = field[v] - one_dot(pto[v], stack3(end_planes(v))).reshape(cz, cy, cx)

    for group in x_copies + [stat_copies[1]]:
        for copy in group:
            copy.wait_recv()
    stz[me[2]] = gathered(stx, gx)
    stat_copies.append(spread(2, lambda t: stz.at[me[2]], stz.at[me[2]], lambda k: ss.at[2, k], lambda k: sr.at[2, k]))

    ext[...] = jnp.transpose(split_dot(halves(mb[...]), halves(xb[...].reshape(wide_x, rows))))
    lane_e = iota((plane4, cx), 1)
    lane_v = jnp.where(lane_e < 96, (lane_e % 32) // 4, -1)
    ends = jnp.concatenate([ext[pl.ds(0, 2 * cy), :], ext[pl.ds((cz - 2) * cy, 2 * cy), :]], axis=0)

    def by_variable(table, a):
        result = None
        for v in range(nv):
            term = one_dot(table[v], stack3(jnp.where(lane_v == v, a, 0.0)))
            result = term if result is None else result + term
        return result

    esend[...] = by_variable(wts, ends)[0:gz * 2 * cy].reshape(gz, 2 * cy, cx)
    e_copies = spread(2, lambda t: esend.at[t], erecv.at[me[2]], lambda k: es.at[k], lambda k: er.at[k])
    ext[...] = ext[...] - by_variable(pto, ends)

    def sides(load):
        before, after = None, None
        for k in range(1, gz):
            q = lax.rem(me[2] + k, gz)
            value = load(q)
            left, right = jnp.where(q < me[2], value, 0.0), jnp.where(q > me[2], value, 0.0)
            before = left if before is None else before + left
            after = right if after is None else after + right
        return jnp.concatenate([before, after], axis=0)

    def doubled(a, lanes):
        high = a.astype(bf16).astype(f32)
        return jnp.where((lanes >= 32) & (lanes < 64), a - high, high).astype(bf16)

    parts = doubled(ext[...], lane_c)
    for v in every:
        field[v] = field[v] - one_dot(parts, cxb[:, v * cx:(v + 1) * cx]).reshape(cz, cy, cx)

    for copy in stat_copies[2]:
        copy.wait_recv()
    final = gathered(stz, gz)
    norm = jnp.sqrt(jnp.sum(final, axis=1, keepdims=True) / float(cells))
    fastest = courant / jnp.max(final, axis=1, keepdims=True)
    stats_out[...] = jnp.broadcast_to(norm, (8, cx))
    time_step = fastest[5:6, :]

    for copy in e_copies:
        copy.wait_recv()
    for v in every:
        for copy in z_copies[v]:
            copy.wait_recv()
    parts = doubled(sides(lambda q: erecv[q]), lane_e)
    shares = [sides(lambda q: zrecv[v, q]) - one_dot(parts, cxb[:, v * cx:(v + 1) * cx]) for v in every]
    for v in every:
        out[v] = (field[v].reshape(rows, cx) - one_dot(pts[v], stack3(shares[v]))) * time_step

    for group in [x_halo, y_halo, z_halo, e_copies] + x_copies + y_copies + z_copies + stat_copies:
        for copy in group:
            copy.wait_send()


def finish(nv, solved, stats, update, norm, sem):
    copies = []
    for v in range(nv):
        copy = pltpu.make_async_copy(solved.at[v], update.at[v], sem.at[v])
        copy.start()
        copies.append(copy)
    for v in range(nv):
        norm[v] = stats[v, 0]
    for copy in copies:
        copy.wait()


def shards(counts, flow_state, advection, inverse_x, inverse_y, inverse_z, reduced_x, reduced_y, reduced_z):
    nv, cz, cy, cx = flow_state.shape
    gx, gy, gz = counts
    rows = cz * cy
    cells = rows * cx * gx * gy * gz
    most = max(counts) - 1
    hbm = pl.BlockSpec(memory_space=pltpu.HBM)
    vmem = pl.BlockSpec(memory_space=pltpu.VMEM)
    dma = pltpu.SemaphoreType.DMA
    pack = -(-4 * nv // 8) * 8
    nc = 2 if gy == 2 else 4
    nd = max(8, gy * nc)
    nz = max(8, 2 * gz)
    width = 12 * cy
    group = cy * min(cz, max(1, 256 // cy))
    out, stats = pl.pallas_call(
        functools.partial(kernel, (counts, nv, cz, cy, cx, cells)),
        out_shape=(pltpu.VMEM((nv, rows, cx), f32), pltpu.VMEM((8, cx), f32)),
        in_specs=[hbm] * 8,
        out_specs=(vmem, vmem),
        scratch_shapes=[
            pltpu.VMEM((nv, (cz + 4) * cy, cx), f32),
            pltpu.VMEM((nv, (cy + 4) * cz, cx), f32),
            pltpu.VMEM((3, (cz + 4) * cy, cx), f32),
            pltpu.VMEM(((cz + 4) * cy, cx), f32),
            pltpu.VMEM((3, pack, rows), f32),
            pltpu.VMEM((nv, rows, cx), f32),
            pltpu.VMEM((nv, rows, cx), f32),
            pltpu.VMEM((nv, cz, cy, cx), f32),
            pltpu.VMEM((nv, rows, cx), f32),
            pltpu.VMEM((rows, cx), f32),
            pltpu.VMEM((nv, nd * cz, 12 * cz), bf16),
            pltpu.VMEM((nv, nz * cy, width), bf16),
            pltpu.VMEM((nv, rows, width), bf16),
            pltpu.VMEM((nv, rows, width), bf16),
            pltpu.VMEM((nv, 8 * cz, 8 * cz), bf16),
            pltpu.VMEM((nv, 8 * cz, 8 * cz), bf16),
            pltpu.VMEM((nv, group, group), bf16),
            pltpu.VMEM((nv, group, group), bf16),
            pltpu.VMEM((nv, 2 * cx, 2 * cx), bf16),
            pltpu.VMEM((nv, cy, nc * cx), f32),
            pltpu.VMEM((cx, gx * pack), f32),
            pltpu.VMEM((cx, nv * cx), f32),
            pltpu.VMEM((cx, nv * cx), bf16),
            pltpu.VMEM((gx, pack, rows), f32),
            pltpu.VMEM((nv, gy, nc * cz, cx), f32),
            pltpu.VMEM((nv, gy, nc * cz, cx), f32),
            pltpu.VMEM((nv, gz, 2 * cy, cx), f32),
            pltpu.VMEM((nv, gz, 2 * cy, cx), f32),
            pltpu.VMEM((gz, 2 * cy, cx), f32),
            pltpu.VMEM((gz, 2 * cy, cx), f32),
            pltpu.VMEM((gx, 8, cx), f32),
            pltpu.VMEM((gy, 8, cx), f32),
            pltpu.VMEM((gz, 8, cx), f32),
            pltpu.VMEM(inverse_x.shape, f32),
            pltpu.VMEM(inverse_y.shape, f32),
            pltpu.VMEM(inverse_z.shape, f32),
            pltpu.VMEM(reduced_x.shape, f32),
            pltpu.VMEM(reduced_y.shape, f32),
            pltpu.VMEM(reduced_z.shape, f32),
            pltpu.SMEM(advection.shape, f32),
            dma((nv,)),
            dma((7,)),
            dma((6,)), dma((6,)),
            dma((gx - 1,)), dma((gx - 1,)),
            dma((nv, gy - 1)), dma((nv, gy - 1)),
            dma((nv, gz - 1)), dma((nv, gz - 1)),
            dma((gz - 1,)), dma((gz - 1,)),
            dma((3, most)), dma((3, most)),
        ],
        compiler_params=pltpu.CompilerParams(
            collective_id=0, has_side_effects=True, vmem_limit_bytes=60 * 1024 * 1024),
    )(flow_state.reshape(nv, rows, cx), advection, inverse_x, inverse_y, inverse_z, reduced_x, reduced_y, reduced_z)
    update, norm = pl.pallas_call(
        functools.partial(finish, nv),
        out_shape=(jax.ShapeDtypeStruct((nv, rows, cx), f32), jax.ShapeDtypeStruct((nv,), f32)),
        in_specs=[vmem, vmem],
        out_specs=(pl.BlockSpec(memory_space=pltpu.HBM), pl.BlockSpec(memory_space=pltpu.SMEM)),
        scratch_shapes=[dma((nv,))],
        compiler_params=pltpu.CompilerParams(vmem_limit_bytes=4 * 1024 * 1024),
    )(out, stats)
    return update.reshape(flow_state.shape), norm


def solution(mesh):
    counts = tuple(mesh.shape[axis] for axis in AXES)
    placed = (P(None, "gz", "gy", "gx"), P(), P(), P(), P(), P(), P(), P())
    return jax.shard_map(
        functools.partial(shards, counts),
        mesh=mesh,
        in_specs=placed,
        out_specs=(P(None, "gz", "gy", "gx"), P()),
        check_vma=False,
    )
```

```python
import functools

import jax
import jax.numpy as jnp
from jax import lax
from jax.experimental import pallas as pl
from jax.experimental.pallas import tpu as pltpu
from jax.sharding import PartitionSpec as P

MESH = pl.DeviceIdType.MESH
HIGHEST = lax.Precision.HIGHEST
gas_ratio = 0.4
courant = 8000.0
damping = 0.0625
fourth_coef = 0.5
AXES = ("gx", "gy", "gz")
f32 = jnp.float32
bf16 = jnp.bfloat16

NN = (((1,), (0,)), ((), ()))
NT = (((1,), (1,)), ((), ()))
TN = (((0,), (0,)), ((), ()))


def exact_dot(a, b, dims=NN):
    return lax.dot_general(a, b, dims, precision=HIGHEST, preferred_element_type=f32)


def one_dot(a, b, dims=NN):
    return lax.dot_general(a, b, dims, preferred_element_type=f32)


def halves(a):
    high = a.astype(bf16)
    low = (a - high.astype(f32)).astype(bf16)
    return high, low


def split_dot(a, b, dims=NN):
    return one_dot(a[0], b[0], dims) + (one_dot(a[0], b[1], dims) + one_dot(a[1], b[0], dims))


def stack3(a):
    high, low = halves(a)
    return jnp.concatenate([high, low, high], axis=0)


def iota(shape, dim):
    return lax.broadcasted_iota(jnp.int32, shape, dim)


def ones_where(mask):
    return jnp.where(mask, 1.0, 0.0).astype(f32)


def primitives(u):
    inverse = 1.0 / u[0]
    velocity = [u[1] * inverse, u[2] * inverse, u[3] * inverse]
    kinetic = 0.5 * (velocity[0] * velocity[0] + velocity[1] * velocity[1] + velocity[2] * velocity[2])
    internal = jnp.maximum(u[4] * inverse - kinetic, 0.25)
    pressure = gas_ratio * u[0] * internal
    return velocity, internal, pressure


def fluxes(u, direction, values=None):
    velocity, internal, pressure = primitives(u) if values is None else values
    carried = velocity[direction]
    found = [u[1 + direction]]
    for component in range(3):
        moment = u[1 + component] * carried
        if component == direction:
            moment = moment + pressure
        found.append(moment)
    found.append((u[4] + pressure) * carried)
    return found


def coupled(col, block, part, speed):
    lower = -0.5 * speed - 4.0 * fourth_coef
    upper = 0.5 * speed - 4.0 * fourth_coef
    value = jnp.where((part == 0) & (col == 4 * block - 2), fourth_coef, 0.0)
    value = jnp.where((part == 0) & (col == 4 * block - 1), lower, value)
    value = jnp.where((part == 1) & (col == 4 * block - 1), fourth_coef, value)
    value = jnp.where((part == 2) & (col == 4 * block + 4), fourth_coef, value)
    value = jnp.where((part == 3) & (col == 4 * block + 4), upper, value)
    return jnp.where((part == 3) & (col == 4 * block + 5), fourth_coef, value).astype(f32)


def face_pick(shape, size, row_dim=0):
    r, c = iota(shape, row_dim), iota(shape, 1 - row_dim)
    return ones_where((r < 4) & (c == jnp.where(r < 2, r, size - 4 + r)))


def kernel(dims, state_h, adv_h, ax_h, ay_h, az_h, rx_h, ry_h, rz_h, out, stats_out,
           uz, uy, vel, prs, hx, res, edge, field, first, ext, wys, wts, pts, pto, kzh, kzl, kyh, kyl, axs, cyt, mb, mw, cxf, cxb,
           xb, ysend, yrecv, zsend, zrecv, esend, erecv, stp, sty,
           ax, ay, az, rx, ry, rz, adv,
           in_sem, aux_sem, halo_send, halo_recv, xs, xr, ys, yr, zs, zr, es, er, ps, pr, ss, sr, joined):
    counts, nv, cz, cy, cx, cells = dims
    gx, gy, gz = counts
    rows = cz * cy
    pack = xb.shape[1]
    nc = 2 if gy == 2 else 4
    plane4 = 4 * cy
    me = [lax.axis_index(axis) for axis in AXES]

    loads = []
    for v in range(nv):
        copy = pltpu.make_async_copy(state_h.at[v], uz.at[v, pl.ds(2 * cy, rows)], in_sem.at[v])
        copy.start()
        loads.append(copy)
    aux = []
    for i, (src, dst) in enumerate([(az_h, az), (ay_h, ay), (ry_h, ry), (rz_h, rz), (rx_h, rx), (adv_h, adv), (ax_h, ax)]):
        copy = pltpu.make_async_copy(src, dst, aux_sem.at[i])
        copy.start()
        aux.append(copy)

    barrier = pltpu.get_barrier_semaphore()
    total = 0
    for axis, count, place in zip(AXES, counts, me):
        for k in range(1, count):
            pl.semaphore_signal(barrier, inc=1, device_id={axis: lax.rem(place + k, count)}, device_id_type=MESH)
            total += 1
    for copy in loads:
        copy.wait()

    lane_c = iota((rows, cx), 1)

    def faces_packed(load):
        packed = jnp.zeros((rows, cx), f32)
        for v in range(nv):
            moved = pltpu.roll(load(v), 4 * v + 2, 1)
            packed = jnp.where(lane_c // 4 == v, moved, packed)
        return packed

    pl.semaphore_wait(barrier, total)
    for k in range(1, gz):
        pl.semaphore_signal(joined, inc=1, device_id={"gz": lax.rem(me[2] + k, gz)}, device_id_type=MESH)

    def ring(axis, slot, down_src, down_dst, up_src, up_dst, far_first=False):
        count, place = counts[axis], me[axis]
        lower = lax.rem(place + count - 1, count)
        upper = lax.rem(place + 1, count)
        down = pltpu.make_async_remote_copy(
            src_ref=down_src, dst_ref=down_dst, send_sem=halo_send.at[slot], recv_sem=halo_recv.at[slot],
            device_id={AXES[axis]: lower}, device_id_type=MESH)
        up = pltpu.make_async_remote_copy(
            src_ref=up_src, dst_ref=up_dst, send_sem=halo_send.at[slot + 1], recv_sem=halo_recv.at[slot + 1],
            device_id={AXES[axis]: upper}, device_id_type=MESH)
        if far_first:
            @pl.when(place == count - 1)
            def _():
                up.start()
                down.start()

            @pl.when(place < count - 1)
            def _():
                down.start()
                up.start()
        else:
            down.start()
            up.start()
        return [down, up]

    def spread(axis, src, dst, send, recv):
        count, place = counts[axis], me[axis]
        copies = []
        for k in range(1, count):
            target = lax.rem(place + k, count)
            copy = pltpu.make_async_remote_copy(
                src_ref=src(target), dst_ref=dst, send_sem=send(k - 1), recv_sem=recv(k - 1),
                device_id={AXES[axis]: target}, device_id_type=MESH)
            copy.start()
            copies.append(copy)
        return copies

    def across(src, dst, send, recv, same_z):
        copies = []
        for kz in range(gz):
            for kx in range(gx):
                if kz == 0 and (kx == 0 or not same_z):
                    continue
                tx, tz = lax.rem(me[0] + kx, gx), lax.rem(me[2] + kz, gz)
                n = kz * gx + kx
                copy = pltpu.make_async_remote_copy(
                    src_ref=src(tz), dst_ref=dst, send_sem=send.at[n], recv_sem=recv.at[n],
                    device_id={"gx": tx, "gz": tz}, device_id_type=MESH)
                copy.start()
                copies.append(copy)
        return copies

    z_halo = ring(2, 4,
                  uz.at[:, pl.ds(2 * cy, 2 * cy)], uz.at[:, pl.ds((cz + 2) * cy, 2 * cy)],
                  uz.at[:, pl.ds(cz * cy, 2 * cy)], uz.at[:, pl.ds(0, 2 * cy)], far_first=True)
    hx[0] = jnp.transpose(faces_packed(lambda v: uz[v, pl.ds(2 * cy, rows), :]))[0:pack]

    x_halo = ring(0, 0, hx.at[0], hx.at[1], hx.at[0], hx.at[2])

    for v in range(nv):
        for y in range(cy):
            uy[v, pl.ds((y + 2) * cz, cz), :] = uz[v, pl.ds(2 * cy + y, cz, stride=cy), :]
    y_halo = ring(1, 2,
                  uy.at[:, pl.ds(2 * cz, 2 * cz)], uy.at[:, pl.ds((cy + 2) * cz, 2 * cz)],
                  uy.at[:, pl.ds(cy * cz, 2 * cz)], uy.at[:, pl.ds(0, 2 * cz)])

    def derive(start, size):
        at = pl.ds(start, size)
        velocity, internal, pressure = primitives([uz[v, at, :] for v in range(nv)])
        for j in range(3):
            vel[j, at, :] = velocity[j]
        prs[at, :] = pressure
        return (jnp.abs(velocity[0]) + jnp.abs(velocity[1]) + jnp.abs(velocity[2])
                + jnp.sqrt(3.0 * 1.4 * gas_ratio * internal))

    chunk = 4 * cy
    top = lax.fori_loop(
        0, rows // chunk,
        lambda i, top: jnp.maximum(top, derive(pl.multiple_of(2 * cy + i * chunk, 8), chunk)),
        jnp.zeros((chunk, cx), f32))

    for copy in aux:
        copy.wait()

    every = range(nv)
    octets = cy // 8
    group = kyh.shape[1]
    planes = group // cy
    groups = cz // planes

    def tall(a, times):
        return jnp.broadcast_to(a[:, None, :], (a.shape[0], times, a.shape[1])).reshape(a.shape[0] * times, a.shape[1])

    def again(a, times):
        return jnp.broadcast_to(a[None], (times,) + a.shape).reshape(times * a.shape[0], a.shape[1])

    size_z = kzh.shape[1]
    spread_z = ones_where(iota((cz, size_z), 1) // 8 == iota((cz, size_z), 0))
    spread_y = ones_where(lax.rem(iota((cy, group), 1), cy) == iota((cy, group), 0))
    keep_z = lax.rem(iota((size_z, size_z), 0), 8) == lax.rem(iota((size_z, size_z), 1), 8)
    keep_y = iota((group, group), 0) // cy == iota((group, group), 1) // cy

    nd = wys.shape[1] // cz
    row_y, col_y = iota((nd, 4 * gy), 0), iota((nd, 4 * gy), 1)
    block_y = row_y // nc
    part_y = row_y % nc + (jnp.where(block_y == 0, 2, 0) if nc == 2 else 0)
    pick_y = ones_where((iota((4 * gy, 8), 0) == 4 * me[1] + iota((4 * gy, 8), 1)) & (iota((4 * gy, 8), 1) < 4))
    width_y = wys.shape[2]
    tiled_y = ones_where(lax.rem(iota((8, width_y), 1), 4 * cz) // cz == iota((8, width_y), 0))
    low_y = iota((1, width_y), 1) >= 8 * cz
    same_z = iota((cz, width_y), 0) == lax.rem(iota((cz, width_y), 1), cz)
    mark_y = iota((cy, nc * cx), 1) // cx
    if nc == 2:
        mark_y = jnp.where(me[1] == 0, cy - 2, 0) + mark_y
    else:
        mark_y = jnp.where(mark_y < 2, mark_y, cy - 4 + mark_y)
    mark_y = ones_where(iota((cy, nc * cx), 0) == mark_y)

    nz = wts.shape[1] // cy
    row_z, col_z = iota((nz, 4 * gz), 0), iota((nz, 4 * gz), 1)
    dest = row_z // 2
    wanted = jnp.where(dest > me[2], 4 * dest - 2, 4 * dest + 4) + row_z % 2
    sel_z = ones_where((dest != me[2]) & (col_z == wanted) & (dest < gz))
    pick_z = ones_where((iota((4 * gz, 8), 0) == 4 * me[2] + iota((4 * gz, 8), 1)) & (iota((4 * gz, 8), 1) < 4))
    width = wts.shape[2]
    tiled = ones_where(lax.rem(iota((8, width), 1), plane4) // cy == iota((8, width), 0))
    low_lane = iota((1, width), 1) >= 2 * plane4
    same_y = lax.rem(iota((cy, width), 1), cy) == iota((cy, width), 0)
    r8, c8 = iota((8, 8), 0), iota((8, 8), 1)

    def stacked(a, low_lane):
        high = a.astype(bf16).astype(f32)
        return jnp.where(low_lane, a - high, high)

    gives_z = [exact_dot(rz[v], pick_z) for v in every]
    gives_y = [exact_dot(ry[v], pick_y) for v in every]
    gives_z = [exact_dot(sel_z, gives_z[v]) for v in every]
    gives_y = [exact_dot(coupled(col_y, block_y, part_y, adv[1, v]), gives_y[v]) for v in every]
    wide_z = [exact_dot(az[v], spread_z) for v in every]
    wide_y = [exact_dot(ay[v], spread_y) for v in every]
    gives_z = [stacked(exact_dot(gives_z[v], tiled), low_lane) for v in every]
    gives_y = [stacked(exact_dot(gives_y[v], tiled_y), low_y) for v in every]
    for v in every:
        cyt[v] = exact_dot(ay[v], mark_y)
        kzh[v], kzl[v] = halves(jnp.where(keep_z, tall(wide_z[v], 8), 0.0))
        kyh[v], kyl[v] = halves(jnp.where(keep_y, again(wide_y[v], planes), 0.0))
        high, low = halves(ax[v])
        axs[v, 0:cx] = jnp.concatenate([high, high], axis=1)
        axs[v, cx:2 * cx] = jnp.concatenate([low, jnp.zeros_like(low)], axis=1)
    for v in every:
        for n in range(nd):
            wys[v, pl.ds(n * cz, cz), :] = jnp.where(same_z, gives_y[v][n:n + 1, :], 0.0).astype(bf16)
        for n in range(nz):
            wts[v, pl.ds(n * cy, cy), :] = jnp.where(same_y, gives_z[v][n:n + 1, :], 0.0).astype(bf16)

    def part(u, direction):
        ahead = fluxes(u[1], direction)
        behind = fluxes(u[-1], direction)
        found = []
        for v in range(nv):
            fourth = u[-2][v] - 4.0 * u[-1][v] + 6.0 * u[0][v] - 4.0 * u[1][v] + u[2][v]
            found.append(-0.5 * (ahead[v] - behind[v]) - damping * fourth)
        return found

    for copy in y_halo:
        copy.wait_recv()

    @pl.loop(0, cy)
    def _(y):
        u = {}
        for off in range(-2, 3):
            at = pl.ds(pl.multiple_of((y + 2 + off) * cz, cz), cz)
            u[off] = [uy[v, at, :] for v in range(nv)]
        found = part(u, 1)
        for v in range(nv):
            res[v, pl.ds(y, cz, stride=cy), :] = found[v]

    for copy in x_halo:
        copy.wait_recv()
    sub4 = iota((4, rows), 0)
    merged = [jnp.where(sub4 < 2, hx[2, 4 * v:4 * v + 4, :], hx[1, 4 * v:4 * v + 4, :]) for v in range(nv)]
    nearest = [hx[0, 4 * v:4 * v + 4, :] for v in range(nv)]
    halo_flux = [a - b for a, b in zip(fluxes(merged, 0), fluxes(nearest, 0))]
    merged = [a - b for a, b in zip(merged, nearest)]
    sub8, lane8 = iota((8, cx), 0), iota((8, cx), 1)

    def at_lane(row, lane, value):
        return jnp.where((sub8 == row) & (lane8 == lane), value, 0.0)

    weights = (at_lane(0, 0, -damping) + at_lane(1, 0, 4.0 * damping) + at_lane(1, 1, -damping)
               + at_lane(2, cx - 2, -damping) + at_lane(2, cx - 1, 4.0 * damping) + at_lane(3, cx - 1, -damping)
               + at_lane(6, cx - 1, -0.5) + at_lane(5, 0, 0.5)).astype(bf16)
    weights = jnp.concatenate([weights, weights], axis=0)
    weights = jnp.concatenate([weights, weights], axis=0)
    for v in range(nv):
        both = jnp.concatenate([merged[v], halo_flux[v]], axis=0)
        high = both.astype(bf16).astype(f32)
        mid = (both - high).astype(bf16).astype(f32)
        parts = jnp.concatenate([high, mid, both - high - mid, jnp.zeros_like(both)], axis=0).astype(bf16)
        edge[v] = one_dot(parts, weights, TN)

    def residual(base, planes, squares):
        size = planes * cy
        here = pl.ds(base + 2 * cy, size)
        vx, pc = vel[0, here, :], prs[here, :]
        around = pl.ds(base + cy, size + 2 * cy)
        vz, pz = vel[2, around, :], prs[around, :]
        found = []
        for v in range(nv):
            u = uz[v, pl.ds(base, size + 4 * cy), :]
            inner = u[cy:size + 3 * cy]
            c = u[2 * cy:size + 2 * cy]
            if v == 0:
                flux_x, flux_z = uz[1, here, :], uz[3, around, :]
            elif v == 4:
                flux_x, flux_z = (c + pc) * vx, (inner + pz) * vz
            else:
                flux_x = c * vx + pc if v == 1 else c * vx
                flux_z = inner * vz + pz if v == 3 else inner * vz
            beside = inner[0:size] + inner[2 * cy:size + 2 * cy]
            beyond = u[0:size] + u[4 * cy:size + 4 * cy]
            along_z = 0.5 * (flux_z[0:size] - flux_z[2 * cy:size + 2 * cy]) + (4.0 * damping * beside - damping * beyond)
            near, half, far = 4.0 * damping * c, 0.5 * flux_x, -damping * c
            along_x = ((pltpu.roll(near - half, cx - 1, 1) + pltpu.roll(near + half, 1, 1))
                       + (pltpu.roll(far, cx - 2, 1) + pltpu.roll(far, 2, 1)))
            at = pl.ds(base, size)
            value = (res[v, at, :] + edge[v, at, :]) + (along_z + along_x) - 12.0 * damping * c
            res[v, at, :] = value
            found.append(squares[v] + jnp.sum((value * value).reshape(planes, cy, cx), axis=0))
        return tuple(found)

    planes_in = next(n for n in (7, 4, 2, 1) if (cz - 4) % n == 0)
    squares = lax.fori_loop(
        0, (cz - 4) // planes_in,
        lambda i, c: residual(pl.multiple_of(2 * cy + i * planes_in * cy, 8), planes_in, c),
        (jnp.zeros((cy, cx), f32),) * nv)
    for copy in z_halo:
        copy.wait_recv()
    derive(0, 2 * cy)
    derive((cz + 2) * cy, 2 * cy)
    squares = residual(0, 2, squares)
    squares = residual((cz - 2) * cy, 2, squares)

    lane_s = iota((1, cx), 1)
    tile = jnp.where(lane_s == nv, jnp.max(top, keepdims=True), 0.0)
    for v in range(nv):
        tile = jnp.where(lane_s == v, jnp.sum(squares[v], keepdims=True), tile)
    sty[me[1]] = tile
    stat_copies = [spread(1, lambda t: sty.at[me[1]], sty.at[me[1]], lambda k: ss.at[k], lambda k: sr.at[k])]

    def gathered(ref, count):
        result = ref[0]
        for q in range(1, count):
            result = jnp.where(lane_s < nv, result + ref[q], jnp.maximum(result, ref[q]))
        return result

    y_copies, z_copies = [], []

    def local_x(v):
        both = one_dot(jnp.concatenate(halves(res[v]), axis=1), axs[v], NT)
        res[v] = both[:, 0:cx] + both[:, cx:2 * cx]

    def local_y(v):
        wide = [jnp.concatenate([a[i * group:(i + 1) * group] for i in range(groups)], axis=1) for a in halves(res[v])]
        solved = split_dot((kyh[v], kyl[v]), wide)
        for i in range(groups):
            first[v, pl.ds(i * group, group), :] = solved[:, i * cx:(i + 1) * cx]

    def send_y(v):
        ends = jnp.concatenate(
            [first[v, pl.ds(mark, cz, stride=cy), :] for mark in (0, 1, cy - 2, cy - 1)], axis=0)
        ysend[v] = one_dot(wys[v], stack3(ends))[0:gy * nc * cz].reshape(gy, nc * cz, cx)
        y_copies.append(spread(1, lambda t: ysend.at[v, t], yrecv.at[v, me[1]],
                               lambda k: ys.at[v, k], lambda k: yr.at[v, k]))

    def solve_z(v):
        for copy in y_copies[v]:
            copy.wait_recv()
        taken = ysend[v, me[1]]
        for k in range(1, gy):
            taken = taken + yrecv[v, lax.rem(me[1] + k, gy)]
        value = first[v].reshape(cz, cy, cx)
        for c in range(nc):
            value = value - cyt[v, :, c * cx:(c + 1) * cx][None] * taken[c * cz:(c + 1) * cz][:, None, :]
        wide = jnp.concatenate(
            [value[:, 8 * i:8 * i + 8, :].reshape(size_z, cx) for i in range(octets)], axis=1)
        solved = split_dot((kzh[v], kzl[v]), halves(wide))
        for i in range(octets):
            field[v, :, 8 * i:8 * i + 8, :] = solved[:, i * cx:(i + 1) * cx].reshape(cz, 8, cx)

    def end_planes(v):
        return jnp.concatenate([field[v, 0:2].reshape(2 * cy, cx), field[v, cz - 2:cz].reshape(2 * cy, cx)], axis=0)

    def send_z(v):
        zsend[v] = one_dot(wts[v], stack3(end_planes(v)))[0:gz * 2 * cy].reshape(gz, 2 * cy, cx)
        z_copies.append(spread(2, lambda t: zsend.at[v, t], zrecv.at[v, me[2]],
                               lambda k: zs.at[v, k], lambda k: zr.at[v, k]))

    for turn in range(nv + 2):
        if turn < nv:
            local_x(turn)
        if turn >= 2:
            solve_z(turn - 2)
        if turn < nv:
            local_y(turn)
        if turn >= 2:
            send_z(turn - 2)
        if turn == 2:
            for copy in stat_copies[0]:
                copy.wait_recv()
            stp[me[2] * gx + me[0]] = gathered(sty, gy)
            pl.semaphore_wait(joined, gz - 1)
            mine = stp.at[me[2] * gx + me[0]]
            stat_copies.append(across(lambda t: mine, mine, ps, pr, True))
        if turn < nv:
            send_y(turn)

    packed = faces_packed(lambda v: field[v].reshape(rows, cx))
    xb[me[0]] = jnp.transpose(packed)[0:pack]
    x_copies = [spread(0, lambda t: xb.at[me[0]], xb.at[me[0]], lambda k: xs.at[k], lambda k: xr.at[k])]

    def by_variable(table, a, variable):
        result = None
        for v in range(nv):
            term = one_dot(table[v], stack3(jnp.where(variable == v, a, 0.0)))
            result = term if result is None else result + term
        return result

    def ends_of(a):
        return jnp.concatenate([a[0:2 * cy], a[rows - 2 * cy:rows]], axis=0)

    lane_e = iota((plane4, cx), 1)
    given = by_variable(wts, ends_of(packed), lane_e // 4)
    eights = 2 * cy // 8
    for t in range(gz):
        piece = given[t * 2 * cy:t * 2 * cy + 8]
        for j in range(1, eights):
            piece = piece + pltpu.roll(given[t * 2 * cy + 8 * j:t * 2 * cy + 8 * j + 8], 32 * j, 1)
        esend[t] = piece
    e_copies = across(lambda t: esend.at[t], erecv.at[me[2] * gx + me[0]], es, er, False)

    mb[...] = jnp.zeros_like(mb)
    mw[...] = jnp.zeros_like(mw)
    cxf[...] = jnp.zeros_like(cxf)
    wide_x = gx * pack
    row_x = iota((8, 4 * gx), 0)
    row_l, col_l = iota((8, 4 * gz), 0), iota((8, 4 * gz), 1)
    sel_lf = ones_where((row_l < 4) & (col_l == 4 * me[2] + jnp.where(row_l < 2, row_l - 2, row_l + 2)))
    near = [exact_dot(sel_lf, rz[v]) for v in every]
    columns_z = [exact_dot(az[v], face_pick((8, cz), cz), NT) for v in every]
    terms = [exact_dot(coupled(iota((8, 4 * gx), 1), me[0], row_x, adv[0, v]), rx[v]) for v in every]

    def to_pack(v, pitch):
        spot = lax.rem(iota((4 * gx, gx * pitch), 1), pitch)
        block = iota((4 * gx, gx * pitch), 1) // pitch
        return ones_where((spot // 4 == v) & (iota((4 * gx, gx * pitch), 0) == 4 * block + lax.rem(spot + 2, 4)))

    square = [exact_dot(near[v], sel_lf, NT) for v in every]
    own = [exact_dot(near[v], pick_z) for v in every]
    placed = [exact_dot(terms[v], to_pack(v, pack)) for v in every]
    wider = [exact_dot(terms[v], to_pack(v, 32)) for v in every]
    columns = [exact_dot(face_pick((8, cx), cx), ax[v], NT) for v in every]
    for v in every:
        high = columns[v].astype(bf16).astype(f32)
        for k in range(3):
            at = pl.ds(4 * v + 32 * k, 4)
            mb[at, :] = placed[v][0:4]
            mw[at, :] = wider[v][0:4]
            cxf[at, v * cx:(v + 1) * cx] = (high if k < 2 else columns[v] - high)[0:4]

    cxb[...] = cxf[...].astype(bf16)

    def mixed(v):
        def e(i, j):
            return square[v][i:i + 1, j:j + 1]

        det_l = e(0, 0) * e(1, 1) - e(0, 1) * e(1, 0)
        det_f = e(2, 2) * e(3, 3) - e(2, 3) * e(3, 2)
        inv_l = 1.0 / jnp.where(me[2] > 0, det_l, 1.0)
        inv_f = 1.0 / jnp.where(me[2] < gz - 1, det_f, 1.0)
        mix = ones_where((r8 == c8) & (r8 < 4))
        for i in range(2):
            for j, value in enumerate([(e(2 + i, 0) * e(1, 1) - e(2 + i, 1) * e(1, 0)) * inv_l,
                                       (e(2 + i, 1) * e(0, 0) - e(2 + i, 0) * e(0, 1)) * inv_l]):
                mix = jnp.where((r8 == 2 + i) & (c8 == j), value, mix)
            for j, value in enumerate([(e(i, 2) * e(3, 3) - e(i, 3) * e(3, 2)) * inv_f,
                                       (e(i, 3) * e(2, 2) - e(i, 2) * e(2, 3)) * inv_f]):
                mix = jnp.where((r8 == i) & (c8 == 2 + j), value, mix)
        return mix

    def weighed(v):
        speed = adv[2, v]
        weigh = jnp.where((r8 == c8) & (r8 < 4), fourth_coef, 0.0)
        weigh = jnp.where((r8 == 0) & (c8 == 1), -0.5 * speed - 4.0 * fourth_coef, weigh)
        return jnp.where((r8 == 3) & (c8 == 2), 0.5 * speed - 4.0 * fourth_coef, weigh).astype(f32)

    own = [exact_dot(weighed(v), own[v]) for v in every]
    peers = [exact_dot(weighed(v), mixed(v)) for v in every]
    own = [exact_dot(own[v], tiled) for v in every]
    peers = [exact_dot(peers[v], tiled) for v in every]
    own = [stacked(exact_dot(columns_z[v], own[v]), low_lane) for v in every]
    peers = [stacked(exact_dot(columns_z[v], peers[v]), low_lane) for v in every]
    for v in every:
        for z in range(cz):
            pto[v, pl.ds(z * cy, cy), :] = jnp.where(same_y, own[v][z:z + 1, :], 0.0).astype(bf16)
            pts[v, pl.ds(z * cy, cy), :] = jnp.where(same_y, peers[v][z:z + 1, :], 0.0).astype(bf16)

    for v in every:
        field[v] = field[v] - one_dot(pto[v], stack3(end_planes(v))).reshape(cz, cy, cx)

    for copy in x_copies[0]:
        copy.wait_recv()
    ext[...] = jnp.transpose(split_dot(halves(mb[...]), halves(xb[...].reshape(wide_x, rows))))
    lane_v = jnp.where(lane_e < 96, (lane_e % 32) // 4, -1)
    ext[...] = ext[...] - by_variable(pto, ends_of(ext), lane_v)

    def sides(load):
        before, after = None, None
        for k in range(1, gz):
            q = lax.rem(me[2] + k, gz)
            value = load(q)
            left, right = jnp.where(q < me[2], value, 0.0), jnp.where(q > me[2], value, 0.0)
            before = left if before is None else before + left
            after = right if after is None else after + right
        return jnp.concatenate([before, after], axis=0)

    def doubled(a, lanes):
        high = a.astype(bf16).astype(f32)
        return jnp.where((lanes >= 32) & (lanes < 64), a - high, high).astype(bf16)

    parts = doubled(ext[...], lane_c)
    for v in every:
        field[v] = field[v] - one_dot(parts, cxb[:, v * cx:(v + 1) * cx]).reshape(cz, cy, cx)

    for copy in stat_copies[1]:
        copy.wait_recv()
    final = gathered(stp, gz * gx)
    stats_out[...] = jnp.broadcast_to(jnp.sqrt(final / float(cells)), (8, cx))
    time_step = courant / final[:, nv:nv + 1]

    for copy in e_copies:
        copy.wait_recv()
    for v in every:
        for copy in z_copies[v]:
            copy.wait_recv()
    lane_8 = iota((8, cx), 1)
    sums = [[None] * gx, [None] * gx]
    for p in range(gx):
        for k in range(1, gz):
            q = lax.rem(me[2] + k, gz)
            value = erecv[q * gx + p]
            for side, term in enumerate([jnp.where(q < me[2], value, 0.0), jnp.where(q > me[2], value, 0.0)]):
                sums[side][p] = term if k == 1 else sums[side][p] + term
    pieces = []
    for side in range(2):
        for j in range(eights):
            piece = jnp.zeros((8, cx), f32)
            for p in range(gx):
                turned = (32 * (p - j)) % cx
                moved = sums[side][p] if turned == 0 else pltpu.roll(sums[side][p], turned, 1)
                piece = jnp.where(lane_8 // 32 == p, moved, piece)
            pieces.append(piece)
    parts = doubled(split_dot(halves(jnp.concatenate(pieces, axis=0)), halves(mw[...]), NT), lane_e)
    shares = [sides(lambda q: zrecv[v, q]) - one_dot(parts, cxb[:, v * cx:(v + 1) * cx]) for v in every]
    for v in every:
        out[v] = (field[v].reshape(rows, cx) - one_dot(pts[v], stack3(shares[v]))) * time_step

    for group in [x_halo, y_halo, z_halo, e_copies] + x_copies + y_copies + z_copies + stat_copies:
        for copy in group:
            copy.wait_send()


def finish(nv, solved, stats, update, norm, sem):
    copies = []
    for v in range(nv):
        copy = pltpu.make_async_copy(solved.at[v], update.at[v], sem.at[v])
        copy.start()
        copies.append(copy)
    for v in range(nv):
        norm[v] = stats[0, v]
    for copy in copies:
        copy.wait()


def shards(counts, flow_state, advection, inverse_x, inverse_y, inverse_z, reduced_x, reduced_y, reduced_z):
    nv, cz, cy, cx = flow_state.shape
    gx, gy, gz = counts
    rows = cz * cy
    cells = rows * cx * gx * gy * gz
    hbm = pl.BlockSpec(memory_space=pltpu.HBM)
    vmem = pl.BlockSpec(memory_space=pltpu.VMEM)
    dma = pltpu.SemaphoreType.DMA
    pack = -(-4 * nv // 8) * 8
    nc = 2 if gy == 2 else 4
    nd = max(8, gy * nc)
    nz = max(8, 2 * gz)
    width = 12 * cy
    group = cy * min(cz, max(1, 256 // cy))
    out, stats = pl.pallas_call(
        functools.partial(kernel, (counts, nv, cz, cy, cx, cells)),
        out_shape=(pltpu.VMEM((nv, rows, cx), f32), pltpu.VMEM((8, cx), f32)),
        in_specs=[hbm] * 8,
        out_specs=(vmem, vmem),
        scratch_shapes=[
            pltpu.VMEM((nv, (cz + 4) * cy, cx), f32),
            pltpu.VMEM((nv, (cy + 4) * cz, cx), f32),
            pltpu.VMEM((3, (cz + 4) * cy, cx), f32),
            pltpu.VMEM(((cz + 4) * cy, cx), f32),
            pltpu.VMEM((3, pack, rows), f32),
            pltpu.VMEM((nv, rows, cx), f32),
            pltpu.VMEM((nv, rows, cx), f32),
            pltpu.VMEM((nv, cz, cy, cx), f32),
            pltpu.VMEM((nv, rows, cx), f32),
            pltpu.VMEM((rows, cx), f32),
            pltpu.VMEM((nv, nd * cz, 12 * cz), bf16),
            pltpu.VMEM((nv, nz * cy, width), bf16),
            pltpu.VMEM((nv, rows, width), bf16),
            pltpu.VMEM((nv, rows, width), bf16),
            pltpu.VMEM((nv, 8 * cz, 8 * cz), bf16),
            pltpu.VMEM((nv, 8 * cz, 8 * cz), bf16),
            pltpu.VMEM((nv, group, group), bf16),
            pltpu.VMEM((nv, group, group), bf16),
            pltpu.VMEM((nv, 2 * cx, 2 * cx), bf16),
            pltpu.VMEM((nv, cy, nc * cx), f32),
            pltpu.VMEM((cx, gx * pack), f32),
            pltpu.VMEM((cx, gx * 32), f32),
            pltpu.VMEM((cx, nv * cx), f32),
            pltpu.VMEM((cx, nv * cx), bf16),
            pltpu.VMEM((gx, pack, rows), f32),
            pltpu.VMEM((nv, gy, nc * cz, cx), f32),
            pltpu.VMEM((nv, gy, nc * cz, cx), f32),
            pltpu.VMEM((nv, gz, 2 * cy, cx), f32),
            pltpu.VMEM((nv, gz, 2 * cy, cx), f32),
            pltpu.VMEM((gz, 8, cx), f32),
            pltpu.VMEM((gz * gx, 8, cx), f32),
            pltpu.VMEM((gz * gx, 1, cx), f32),
            pltpu.VMEM((gy, 1, cx), f32),
            pltpu.VMEM(inverse_x.shape, f32),
            pltpu.VMEM(inverse_y.shape, f32),
            pltpu.VMEM(inverse_z.shape, f32),
            pltpu.VMEM(reduced_x.shape, f32),
            pltpu.VMEM(reduced_y.shape, f32),
            pltpu.VMEM(reduced_z.shape, f32),
            pltpu.SMEM(advection.shape, f32),
            dma((nv,)),
            dma((7,)),
            dma((6,)), dma((6,)),
            dma((gx - 1,)), dma((gx - 1,)),
            dma((nv, gy - 1)), dma((nv, gy - 1)),
            dma((nv, gz - 1)), dma((nv, gz - 1)),
            dma((gz * gx,)), dma((gz * gx,)),
            dma((gz * gx,)), dma((gz * gx,)),
            dma((gy - 1,)), dma((gy - 1,)),
            pltpu.SemaphoreType.REGULAR,
        ],
        compiler_params=pltpu.CompilerParams(
            collective_id=0, has_side_effects=True, vmem_limit_bytes=60 * 1024 * 1024),
    )(flow_state.reshape(nv, rows, cx), advection, inverse_x, inverse_y, inverse_z, reduced_x, reduced_y, reduced_z)
    update, norm = pl.pallas_call(
        functools.partial(finish, nv),
        out_shape=(jax.ShapeDtypeStruct((nv, rows, cx), f32), jax.ShapeDtypeStruct((nv,), f32)),
        in_specs=[vmem, vmem],
        out_specs=(pl.BlockSpec(memory_space=pltpu.HBM), pl.BlockSpec(memory_space=pltpu.SMEM)),
        scratch_shapes=[dma((nv,))],
        compiler_params=pltpu.CompilerParams(vmem_limit_bytes=4 * 1024 * 1024),
    )(out, stats)
    return update.reshape(flow_state.shape), norm


def solution(mesh):
    counts = tuple(mesh.shape[axis] for axis in AXES)
    placed = (P(None, "gz", "gy", "gx"), P(), P(), P(), P(), P(), P(), P())
    return jax.shard_map(
        functools.partial(shards, counts),
        mesh=mesh,
        in_specs=placed,
        out_specs=(P(None, "gz", "gy", "gx"), P()),
        check_vma=False,
    )
```

```python
import functools

import jax
import jax.numpy as jnp
from jax import lax
from jax.experimental import pallas as pl
from jax.experimental.pallas import tpu as pltpu
from jax.sharding import PartitionSpec as P

MESH = pl.DeviceIdType.MESH
HIGHEST = lax.Precision.HIGHEST
gas_ratio = 0.4
courant = 8000.0
damping = 0.0625
fourth_coef = 0.5
AXES = ("gx", "gy", "gz")
f32 = jnp.float32
bf16 = jnp.bfloat16

NN = (((1,), (0,)), ((), ()))
NT = (((1,), (1,)), ((), ()))
TN = (((0,), (0,)), ((), ()))


def exact_dot(a, b, dims=NN):
    return lax.dot_general(a, b, dims, precision=HIGHEST, preferred_element_type=f32)


def one_dot(a, b, dims=NN):
    return lax.dot_general(a, b, dims, preferred_element_type=f32)


def halves(a):
    high = a.astype(bf16)
    low = (a - high.astype(f32)).astype(bf16)
    return high, low


def split_dot(a, b, dims=NN):
    return one_dot(a[0], b[0], dims) + (one_dot(a[0], b[1], dims) + one_dot(a[1], b[0], dims))


def stack3(a):
    high, low = halves(a)
    return jnp.concatenate([high, low, high], axis=0)


def iota(shape, dim):
    return lax.broadcasted_iota(jnp.int32, shape, dim)


def ones_where(mask):
    return jnp.where(mask, 1.0, 0.0).astype(f32)


def primitives(u):
    inverse = 1.0 / u[0]
    velocity = [u[1] * inverse, u[2] * inverse, u[3] * inverse]
    kinetic = 0.5 * (velocity[0] * velocity[0] + velocity[1] * velocity[1] + velocity[2] * velocity[2])
    internal = jnp.maximum(u[4] * inverse - kinetic, 0.25)
    pressure = gas_ratio * u[0] * internal
    return velocity, internal, pressure


def fluxes(u, direction, values=None):
    velocity, internal, pressure = primitives(u) if values is None else values
    carried = velocity[direction]
    found = [u[1 + direction]]
    for component in range(3):
        moment = u[1 + component] * carried
        if component == direction:
            moment = moment + pressure
        found.append(moment)
    found.append((u[4] + pressure) * carried)
    return found


def coupled(col, block, part, speed):
    lower = -0.5 * speed - 4.0 * fourth_coef
    upper = 0.5 * speed - 4.0 * fourth_coef
    value = jnp.where((part == 0) & (col == 4 * block - 2), fourth_coef, 0.0)
    value = jnp.where((part == 0) & (col == 4 * block - 1), lower, value)
    value = jnp.where((part == 1) & (col == 4 * block - 1), fourth_coef, value)
    value = jnp.where((part == 2) & (col == 4 * block + 4), fourth_coef, value)
    value = jnp.where((part == 3) & (col == 4 * block + 4), upper, value)
    return jnp.where((part == 3) & (col == 4 * block + 5), fourth_coef, value).astype(f32)


def face_pick(shape, size, row_dim=0):
    r, c = iota(shape, row_dim), iota(shape, 1 - row_dim)
    return ones_where((r < 4) & (c == jnp.where(r < 2, r, size - 4 + r)))


def kernel(dims, state_h, adv_h, ax_h, ay_h, az_h, rx_h, ry_h, rz_h, out, stats_out,
           uz, uy, vel, prs, hx, res, edge, field, first, ext, wys, wts, pts, pto, kzh, kzl, kyh, kyl, axs, cyt, mb, mw, cxf, cxb,
           xb, ysend, yrecv, zsend, zrecv, esend, erecv, stp, sty,
           ax, ay, az, rx, ry, rz, adv,
           in_sem, aux_sem, halo_send, halo_recv, xs, xr, ys, yr, zs, zr, es, er, ps, pr, ss, sr, joined):
    counts, nv, cz, cy, cx, cells = dims
    gx, gy, gz = counts
    rows = cz * cy
    pack = xb.shape[1]
    nc = 2 if gy == 2 else 4
    plane4 = 4 * cy
    me = [lax.axis_index(axis) for axis in AXES]

    loads = []
    for v in range(nv):
        copy = pltpu.make_async_copy(state_h.at[v], uz.at[v, pl.ds(2 * cy, rows)], in_sem.at[v])
        copy.start()
        loads.append(copy)
    aux = []
    for i, (src, dst) in enumerate([(az_h, az), (ay_h, ay), (ry_h, ry), (rz_h, rz), (rx_h, rx), (adv_h, adv), (ax_h, ax)]):
        copy = pltpu.make_async_copy(src, dst, aux_sem.at[i])
        copy.start()
        aux.append(copy)

    barrier = pltpu.get_barrier_semaphore()
    total = 0
    for axis, count, place in zip(AXES, counts, me):
        for k in range(1, count):
            pl.semaphore_signal(barrier, inc=1, device_id={axis: lax.rem(place + k, count)}, device_id_type=MESH)
            total += 1
    for copy in loads:
        copy.wait()

    lane_c = iota((rows, cx), 1)

    def faces_packed(load):
        packed = jnp.zeros((rows, cx), f32)
        for v in range(nv):
            moved = pltpu.roll(load(v), 4 * v + 2, 1)
            packed = jnp.where(lane_c // 4 == v, moved, packed)
        return packed

    pl.semaphore_wait(barrier, total)
    for k in range(1, gz):
        pl.semaphore_signal(joined, inc=1, device_id={"gz": lax.rem(me[2] + k, gz)}, device_id_type=MESH)

    def ring(axis, slot, down_src, down_dst, up_src, up_dst, far_first=False):
        count, place = counts[axis], me[axis]
        lower = lax.rem(place + count - 1, count)
        upper = lax.rem(place + 1, count)
        down = pltpu.make_async_remote_copy(
            src_ref=down_src, dst_ref=down_dst, send_sem=halo_send.at[slot], recv_sem=halo_recv.at[slot],
            device_id={AXES[axis]: lower}, device_id_type=MESH)
        up = pltpu.make_async_remote_copy(
            src_ref=up_src, dst_ref=up_dst, send_sem=halo_send.at[slot + 1], recv_sem=halo_recv.at[slot + 1],
            device_id={AXES[axis]: upper}, device_id_type=MESH)
        if far_first:
            @pl.when(place == count - 1)
            def _():
                up.start()
                down.start()

            @pl.when(place < count - 1)
            def _():
                down.start()
                up.start()
        else:
            down.start()
            up.start()
        return [down, up]

    def spread(axis, src, dst, send, recv):
        count, place = counts[axis], me[axis]
        copies = []
        for k in range(1, count):
            target = lax.rem(place + k, count)
            copy = pltpu.make_async_remote_copy(
                src_ref=src(target), dst_ref=dst, send_sem=send(k - 1), recv_sem=recv(k - 1),
                device_id={AXES[axis]: target}, device_id_type=MESH)
            copy.start()
            copies.append(copy)
        return copies

    def across(src, dst, send, recv, same_z):
        copies = []
        for kz in range(gz):
            for kx in range(gx):
                if kz == 0 and (kx == 0 or not same_z):
                    continue
                tx, tz = lax.rem(me[0] + kx, gx), lax.rem(me[2] + kz, gz)
                n = kz * gx + kx
                copy = pltpu.make_async_remote_copy(
                    src_ref=src(tz), dst_ref=dst, send_sem=send.at[n], recv_sem=recv.at[n],
                    device_id={"gx": tx, "gz": tz}, device_id_type=MESH)
                copy.start()
                copies.append(copy)
        return copies

    z_halo = ring(2, 4,
                  uz.at[:, pl.ds(2 * cy, 2 * cy)], uz.at[:, pl.ds((cz + 2) * cy, 2 * cy)],
                  uz.at[:, pl.ds(cz * cy, 2 * cy)], uz.at[:, pl.ds(0, 2 * cy)], far_first=True)
    hx[0] = jnp.transpose(faces_packed(lambda v: uz[v, pl.ds(2 * cy, rows), :]))[0:pack]

    x_halo = ring(0, 0, hx.at[0], hx.at[1], hx.at[0], hx.at[2])

    for v in range(nv):
        for y in range(cy):
            uy[v, pl.ds((y + 2) * cz, cz), :] = uz[v, pl.ds(2 * cy + y, cz, stride=cy), :]
    y_halo = ring(1, 2,
                  uy.at[:, pl.ds(2 * cz, 2 * cz)], uy.at[:, pl.ds((cy + 2) * cz, 2 * cz)],
                  uy.at[:, pl.ds(cy * cz, 2 * cz)], uy.at[:, pl.ds(0, 2 * cz)])

    def derive(start, size):
        at = pl.ds(start, size)
        velocity, internal, pressure = primitives([uz[v, at, :] for v in range(nv)])
        for j in range(3):
            vel[j, at, :] = velocity[j]
        prs[at, :] = pressure
        return (jnp.abs(velocity[0]) + jnp.abs(velocity[1]) + jnp.abs(velocity[2])
                + jnp.sqrt(3.0 * 1.4 * gas_ratio * internal))

    chunk = 4 * cy
    top = lax.fori_loop(
        0, rows // chunk,
        lambda i, top: jnp.maximum(top, derive(pl.multiple_of(2 * cy + i * chunk, 8), chunk)),
        jnp.zeros((chunk, cx), f32))

    for copy in aux:
        copy.wait()

    every = range(nv)
    octets = cy // 8
    group = kyh.shape[1]
    planes = group // cy
    groups = cz // planes

    def tall(a, times):
        return jnp.broadcast_to(a[:, None, :], (a.shape[0], times, a.shape[1])).reshape(a.shape[0] * times, a.shape[1])

    def again(a, times):
        return jnp.broadcast_to(a[None], (times,) + a.shape).reshape(times * a.shape[0], a.shape[1])

    size_z = kzh.shape[1]
    spread_z = ones_where(iota((cz, size_z), 1) // 8 == iota((cz, size_z), 0))
    spread_y = ones_where(lax.rem(iota((cy, group), 1), cy) == iota((cy, group), 0))
    keep_z = lax.rem(iota((size_z, size_z), 0), 8) == lax.rem(iota((size_z, size_z), 1), 8)
    keep_y = iota((group, group), 0) // cy == iota((group, group), 1) // cy

    nd = wys.shape[1] // cz
    row_y, col_y = iota((nd, 4 * gy), 0), iota((nd, 4 * gy), 1)
    block_y = row_y // nc
    part_y = row_y % nc + (jnp.where(block_y == 0, 2, 0) if nc == 2 else 0)
    pick_y = ones_where((iota((4 * gy, 8), 0) == 4 * me[1] + iota((4 * gy, 8), 1)) & (iota((4 * gy, 8), 1) < 4))
    width_y = wys.shape[2]
    tiled_y = ones_where(lax.rem(iota((8, width_y), 1), 4 * cz) // cz == iota((8, width_y), 0))
    low_y = iota((1, width_y), 1) >= 8 * cz
    same_z = iota((cz, width_y), 0) == lax.rem(iota((cz, width_y), 1), cz)
    mark_y = iota((cy, nc * cx), 1) // cx
    if nc == 2:
        mark_y = jnp.where(me[1] == 0, cy - 2, 0) + mark_y
    else:
        mark_y = jnp.where(mark_y < 2, mark_y, cy - 4 + mark_y)
    mark_y = ones_where(iota((cy, nc * cx), 0) == mark_y)

    nz = wts.shape[1] // cy
    row_z, col_z = iota((nz, 4 * gz), 0), iota((nz, 4 * gz), 1)
    dest = row_z // 2
    wanted = jnp.where(dest > me[2], 4 * dest - 2, 4 * dest + 4) + row_z % 2
    sel_z = ones_where((dest != me[2]) & (col_z == wanted) & (dest < gz))
    pick_z = ones_where((iota((4 * gz, 8), 0) == 4 * me[2] + iota((4 * gz, 8), 1)) & (iota((4 * gz, 8), 1) < 4))
    width = wts.shape[2]
    tiled = ones_where(lax.rem(iota((8, width), 1), plane4) // cy == iota((8, width), 0))
    low_lane = iota((1, width), 1) >= 2 * plane4
    same_y = lax.rem(iota((cy, width), 1), cy) == iota((cy, width), 0)
    r8, c8 = iota((8, 8), 0), iota((8, 8), 1)

    def stacked(a, low_lane):
        high = a.astype(bf16).astype(f32)
        return jnp.where(low_lane, a - high, high)

    gives_z = [exact_dot(rz[v], pick_z) for v in every]
    gives_y = [exact_dot(ry[v], pick_y) for v in every]
    gives_z = [exact_dot(sel_z, gives_z[v]) for v in every]
    gives_y = [exact_dot(coupled(col_y, block_y, part_y, adv[1, v]), gives_y[v]) for v in every]
    wide_z = [exact_dot(az[v], spread_z) for v in every]
    wide_y = [exact_dot(ay[v], spread_y) for v in every]
    gives_z = [stacked(exact_dot(gives_z[v], tiled), low_lane) for v in every]
    gives_y = [stacked(exact_dot(gives_y[v], tiled_y), low_y) for v in every]
    for v in every:
        cyt[v] = exact_dot(ay[v], mark_y)
        kzh[v], kzl[v] = halves(jnp.where(keep_z, tall(wide_z[v], 8), 0.0))
        kyh[v], kyl[v] = halves(jnp.where(keep_y, again(wide_y[v], planes), 0.0))
        high, low = halves(ax[v])
        axs[v, 0:cx] = jnp.concatenate([high, high], axis=1)
        axs[v, cx:2 * cx] = jnp.concatenate([low, jnp.zeros_like(low)], axis=1)
    for v in every:
        for n in range(nd):
            wys[v, pl.ds(n * cz, cz), :] = jnp.where(same_z, gives_y[v][n:n + 1, :], 0.0).astype(bf16)
        for n in range(nz):
            wts[v, pl.ds(n * cy, cy), :] = jnp.where(same_y, gives_z[v][n:n + 1, :], 0.0).astype(bf16)

    def part(u, direction):
        ahead = fluxes(u[1], direction)
        behind = fluxes(u[-1], direction)
        found = []
        for v in range(nv):
            fourth = u[-2][v] - 4.0 * u[-1][v] + 6.0 * u[0][v] - 4.0 * u[1][v] + u[2][v]
            found.append(-0.5 * (ahead[v] - behind[v]) - damping * fourth)
        return found

    for copy in y_halo:
        copy.wait_recv()

    @pl.loop(0, cy)
    def _(y):
        u = {}
        for off in range(-2, 3):
            at = pl.ds(pl.multiple_of((y + 2 + off) * cz, cz), cz)
            u[off] = [uy[v, at, :] for v in range(nv)]
        found = part(u, 1)
        for v in range(nv):
            res[v, pl.ds(y, cz, stride=cy), :] = found[v]

    for copy in x_halo:
        copy.wait_recv()
    sub4 = iota((4, rows), 0)
    merged = [jnp.where(sub4 < 2, hx[2, 4 * v:4 * v + 4, :], hx[1, 4 * v:4 * v + 4, :]) for v in range(nv)]
    nearest = [hx[0, 4 * v:4 * v + 4, :] for v in range(nv)]
    halo_flux = [a - b for a, b in zip(fluxes(merged, 0), fluxes(nearest, 0))]
    merged = [a - b for a, b in zip(merged, nearest)]
    sub8, lane8 = iota((8, cx), 0), iota((8, cx), 1)

    def at_lane(row, lane, value):
        return jnp.where((sub8 == row) & (lane8 == lane), value, 0.0)

    weights = (at_lane(0, 0, -damping) + at_lane(1, 0, 4.0 * damping) + at_lane(1, 1, -damping)
               + at_lane(2, cx - 2, -damping) + at_lane(2, cx - 1, 4.0 * damping) + at_lane(3, cx - 1, -damping)
               + at_lane(6, cx - 1, -0.5) + at_lane(5, 0, 0.5)).astype(bf16)
    weights = jnp.concatenate([weights, weights], axis=0)
    weights = jnp.concatenate([weights, weights], axis=0)
    for v in range(nv):
        both = jnp.concatenate([merged[v], halo_flux[v]], axis=0)
        high = both.astype(bf16).astype(f32)
        mid = (both - high).astype(bf16).astype(f32)
        parts = jnp.concatenate([high, mid, both - high - mid, jnp.zeros_like(both)], axis=0).astype(bf16)
        edge[v] = one_dot(parts, weights, TN)

    def residual(base, planes, squares, which=None):
        size = planes * cy
        here = pl.ds(base + 2 * cy, size)
        vx, pc = vel[0, here, :], prs[here, :]
        around = pl.ds(base + cy, size + 2 * cy)
        vz, pz = vel[2, around, :], prs[around, :]
        found = []
        for i, v in enumerate(range(nv) if which is None else [which]):
            u = uz[v, pl.ds(base, size + 4 * cy), :]
            inner = u[cy:size + 3 * cy]
            c = u[2 * cy:size + 2 * cy]
            if v == 0:
                flux_x, flux_z = uz[1, here, :], uz[3, around, :]
            elif v == 4:
                flux_x, flux_z = (c + pc) * vx, (inner + pz) * vz
            else:
                flux_x = c * vx + pc if v == 1 else c * vx
                flux_z = inner * vz + pz if v == 3 else inner * vz
            beside = inner[0:size] + inner[2 * cy:size + 2 * cy]
            beyond = u[0:size] + u[4 * cy:size + 4 * cy]
            along_z = 0.5 * (flux_z[0:size] - flux_z[2 * cy:size + 2 * cy]) + (4.0 * damping * beside - damping * beyond)
            near, half, far = 4.0 * damping * c, 0.5 * flux_x, -damping * c
            along_x = ((pltpu.roll(near - half, cx - 1, 1) + pltpu.roll(near + half, 1, 1))
                       + (pltpu.roll(far, cx - 2, 1) + pltpu.roll(far, 2, 1)))
            at = pl.ds(base, size)
            value = (res[v, at, :] + edge[v, at, :]) + (along_z + along_x) - 12.0 * damping * c
            res[v, at, :] = value
            found.append(squares[i] + jnp.sum((value * value).reshape(planes, cy, cx), axis=0))
        return tuple(found)

    planes_in = next(n for n in (7, 4, 2, 1) if (cz - 4) % n == 0)
    planes_in = next(n for n in (28, 4, 2, 1) if (cz - 4) % n == 0)
    squares = []
    for v in every:
        squares += lax.fori_loop(
            0, (cz - 4) // planes_in,
            lambda i, c: residual(pl.multiple_of(2 * cy + i * planes_in * cy, 8), planes_in, c, v),
            (jnp.zeros((cy, cx), f32),))
    for copy in z_halo:
        copy.wait_recv()
    derive(0, 2 * cy)
    derive((cz + 2) * cy, 2 * cy)
    squares = residual(0, 2, squares)
    squares = residual((cz - 2) * cy, 2, squares)

    lane_s = iota((1, cx), 1)
    tile = jnp.where(lane_s == nv, jnp.max(top, keepdims=True), 0.0)
    for v in range(nv):
        tile = jnp.where(lane_s == v, jnp.sum(squares[v], keepdims=True), tile)
    sty[me[1]] = tile
    stat_copies = [spread(1, lambda t: sty.at[me[1]], sty.at[me[1]], lambda k: ss.at[k], lambda k: sr.at[k])]

    def gathered(ref, count):
        result = ref[0]
        for q in range(1, count):
            result = jnp.where(lane_s < nv, result + ref[q], jnp.maximum(result, ref[q]))
        return result

    y_copies, z_copies = [], []

    def local_x(v):
        both = one_dot(jnp.concatenate(halves(res[v]), axis=1), axs[v], NT)
        res[v] = both[:, 0:cx] + both[:, cx:2 * cx]

    def local_y(v):
        wide = [jnp.concatenate([a[i * group:(i + 1) * group] for i in range(groups)], axis=1) for a in halves(res[v])]
        solved = split_dot((kyh[v], kyl[v]), wide)
        for i in range(groups):
            first[v, pl.ds(i * group, group), :] = solved[:, i * cx:(i + 1) * cx]

    def send_y(v):
        ends = jnp.concatenate(
            [first[v, pl.ds(mark, cz, stride=cy), :] for mark in (0, 1, cy - 2, cy - 1)], axis=0)
        ysend[v] = one_dot(wys[v], stack3(ends))[0:gy * nc * cz].reshape(gy, nc * cz, cx)
        y_copies.append(spread(1, lambda t: ysend.at[v, t], yrecv.at[v, me[1]],
                               lambda k: ys.at[v, k], lambda k: yr.at[v, k]))

    def solve_z(v):
        for copy in y_copies[v]:
            copy.wait_recv()
        taken = ysend[v, me[1]]
        for k in range(1, gy):
            taken = taken + yrecv[v, lax.rem(me[1] + k, gy)]
        value = first[v].reshape(cz, cy, cx)
        for c in range(nc):
            value = value - cyt[v, :, c * cx:(c + 1) * cx][None] * taken[c * cz:(c + 1) * cz][:, None, :]
        wide = jnp.concatenate(
            [value[:, 8 * i:8 * i + 8, :].reshape(size_z, cx) for i in range(octets)], axis=1)
        solved = split_dot((kzh[v], kzl[v]), halves(wide))
        for i in range(octets):
            field[v, :, 8 * i:8 * i + 8, :] = solved[:, i * cx:(i + 1) * cx].reshape(cz, 8, cx)

    def end_planes(v):
        return jnp.concatenate([field[v, 0:2].reshape(2 * cy, cx), field[v, cz - 2:cz].reshape(2 * cy, cx)], axis=0)

    def send_z(v):
        zsend[v] = one_dot(wts[v], stack3(end_planes(v)))[0:gz * 2 * cy].reshape(gz, 2 * cy, cx)
        z_copies.append(spread(2, lambda t: zsend.at[v, t], zrecv.at[v, me[2]],
                               lambda k: zs.at[v, k], lambda k: zr.at[v, k]))

    for turn in range(nv + 2):
        if turn < nv:
            local_x(turn)
        if turn >= 2:
            solve_z(turn - 2)
        if turn < nv:
            local_y(turn)
        if turn >= 2:
            send_z(turn - 2)
        if turn == 2:
            for copy in stat_copies[0]:
                copy.wait_recv()
            stp[me[2] * gx + me[0]] = gathered(sty, gy)
            pl.semaphore_wait(joined, gz - 1)
            mine = stp.at[me[2] * gx + me[0]]
            stat_copies.append(across(lambda t: mine, mine, ps, pr, True))
        if turn < nv:
            send_y(turn)

    packed = faces_packed(lambda v: field[v].reshape(rows, cx))
    xb[me[0]] = jnp.transpose(packed)[0:pack]
    x_copies = [spread(0, lambda t: xb.at[me[0]], xb.at[me[0]], lambda k: xs.at[k], lambda k: xr.at[k])]

    def by_variable(table, a, variable):
        result = None
        for v in range(nv):
            term = one_dot(table[v], stack3(jnp.where(variable == v, a, 0.0)))
            result = term if result is None else result + term
        return result

    def ends_of(a):
        return jnp.concatenate([a[0:2 * cy], a[rows - 2 * cy:rows]], axis=0)

    lane_e = iota((plane4, cx), 1)
    given = by_variable(wts, ends_of(packed), lane_e // 4)
    eights = 2 * cy // 8
    for t in range(gz):
        piece = given[t * 2 * cy:t * 2 * cy + 8]
        for j in range(1, eights):
            piece = piece + pltpu.roll(given[t * 2 * cy + 8 * j:t * 2 * cy + 8 * j + 8], 32 * j, 1)
        esend[t] = piece
    e_copies = across(lambda t: esend.at[t], erecv.at[me[2] * gx + me[0]], es, er, False)

    mb[...] = jnp.zeros_like(mb)
    mw[...] = jnp.zeros_like(mw)
    cxf[...] = jnp.zeros_like(cxf)
    wide_x = gx * pack
    row_x = iota((8, 4 * gx), 0)
    row_l, col_l = iota((8, 4 * gz), 0), iota((8, 4 * gz), 1)
    sel_lf = ones_where((row_l < 4) & (col_l == 4 * me[2] + jnp.where(row_l < 2, row_l - 2, row_l + 2)))
    near = [exact_dot(sel_lf, rz[v]) for v in every]
    columns_z = [exact_dot(az[v], face_pick((8, cz), cz), NT) for v in every]
    terms = [exact_dot(coupled(iota((8, 4 * gx), 1), me[0], row_x, adv[0, v]), rx[v]) for v in every]

    def to_pack(v, pitch):
        spot = lax.rem(iota((4 * gx, gx * pitch), 1), pitch)
        block = iota((4 * gx, gx * pitch), 1) // pitch
        return ones_where((spot // 4 == v) & (iota((4 * gx, gx * pitch), 0) == 4 * block + lax.rem(spot + 2, 4)))

    square = [exact_dot(near[v], sel_lf, NT) for v in every]
    own = [exact_dot(near[v], pick_z) for v in every]
    placed = [exact_dot(terms[v], to_pack(v, pack)) for v in every]
    wider = [exact_dot(terms[v], to_pack(v, 32)) for v in every]
    columns = [exact_dot(face_pick((8, cx), cx), ax[v], NT) for v in every]
    for v in every:
        high = columns[v].astype(bf16).astype(f32)
        for k in range(3):
            at = pl.ds(4 * v + 32 * k, 4)
            mb[at, :] = placed[v][0:4]
            mw[at, :] = wider[v][0:4]
            cxf[at, v * cx:(v + 1) * cx] = (high if k < 2 else columns[v] - high)[0:4]

    cxb[...] = cxf[...].astype(bf16)

    def mixed(v):
        def e(i, j):
            return square[v][i:i + 1, j:j + 1]

        det_l = e(0, 0) * e(1, 1) - e(0, 1) * e(1, 0)
        det_f = e(2, 2) * e(3, 3) - e(2, 3) * e(3, 2)
        inv_l = 1.0 / jnp.where(me[2] > 0, det_l, 1.0)
        inv_f = 1.0 / jnp.where(me[2] < gz - 1, det_f, 1.0)
        mix = ones_where((r8 == c8) & (r8 < 4))
        for i in range(2):
            for j, value in enumerate([(e(2 + i, 0) * e(1, 1) - e(2 + i, 1) * e(1, 0)) * inv_l,
                                       (e(2 + i, 1) * e(0, 0) - e(2 + i, 0) * e(0, 1)) * inv_l]):
                mix = jnp.where((r8 == 2 + i) & (c8 == j), value, mix)
            for j, value in enumerate([(e(i, 2) * e(3, 3) - e(i, 3) * e(3, 2)) * inv_f,
                                       (e(i, 3) * e(2, 2) - e(i, 2) * e(2, 3)) * inv_f]):
                mix = jnp.where((r8 == i) & (c8 == 2 + j), value, mix)
        return mix

    def weighed(v):
        speed = adv[2, v]
        weigh = jnp.where((r8 == c8) & (r8 < 4), fourth_coef, 0.0)
        weigh = jnp.where((r8 == 0) & (c8 == 1), -0.5 * speed - 4.0 * fourth_coef, weigh)
        return jnp.where((r8 == 3) & (c8 == 2), 0.5 * speed - 4.0 * fourth_coef, weigh).astype(f32)

    own = [exact_dot(weighed(v), own[v]) for v in every]
    peers = [exact_dot(weighed(v), mixed(v)) for v in every]
    own = [exact_dot(own[v], tiled) for v in every]
    peers = [exact_dot(peers[v], tiled) for v in every]
    own = [stacked(exact_dot(columns_z[v], own[v]), low_lane) for v in every]
    peers = [stacked(exact_dot(columns_z[v], peers[v]), low_lane) for v in every]
    for v in every:
        for z in range(cz):
            pto[v, pl.ds(z * cy, cy), :] = jnp.where(same_y, own[v][z:z + 1, :], 0.0).astype(bf16)
            pts[v, pl.ds(z * cy, cy), :] = jnp.where(same_y, peers[v][z:z + 1, :], 0.0).astype(bf16)

    for v in every:
        field[v] = field[v] - one_dot(pto[v], stack3(end_planes(v))).reshape(cz, cy, cx)

    for copy in x_copies[0]:
        copy.wait_recv()
    ext[...] = jnp.transpose(split_dot(halves(mb[...]), halves(xb[...].reshape(wide_x, rows))))
    lane_v = jnp.where(lane_e < 96, (lane_e % 32) // 4, -1)
    ext[...] = ext[...] - by_variable(pto, ends_of(ext), lane_v)

    def sides(load):
        before, after = None, None
        for k in range(1, gz):
            q = lax.rem(me[2] + k, gz)
            value = load(q)
            left, right = jnp.where(q < me[2], value, 0.0), jnp.where(q > me[2], value, 0.0)
            before = left if before is None else before + left
            after = right if after is None else after + right
        return jnp.concatenate([before, after], axis=0)

    def doubled(a, lanes):
        high = a.astype(bf16).astype(f32)
        return jnp.where((lanes >= 32) & (lanes < 64), a - high, high).astype(bf16)

    parts = doubled(ext[...], lane_c)
    for v in every:
        field[v] = field[v] - one_dot(parts, cxb[:, v * cx:(v + 1) * cx]).reshape(cz, cy, cx)

    for copy in stat_copies[1]:
        copy.wait_recv()
    final = gathered(stp, gz * gx)
    stats_out[...] = jnp.broadcast_to(jnp.sqrt(final / float(cells)), (8, cx))
    time_step = courant / final[:, nv:nv + 1]

    for copy in e_copies:
        copy.wait_recv()
    for v in every:
        for copy in z_copies[v]:
            copy.wait_recv()
    lane_8 = iota((8, cx), 1)
    sums = [[None] * gx, [None] * gx]
    for p in range(gx):
        for k in range(1, gz):
            q = lax.rem(me[2] + k, gz)
            value = erecv[q * gx + p]
            for side, term in enumerate([jnp.where(q < me[2], value, 0.0), jnp.where(q > me[2], value, 0.0)]):
                sums[side][p] = term if k == 1 else sums[side][p] + term
    pieces = []
    for side in range(2):
        for j in range(eights):
            piece = jnp.zeros((8, cx), f32)
            for p in range(gx):
                turned = (32 * (p - j)) % cx
                moved = sums[side][p] if turned == 0 else pltpu.roll(sums[side][p], turned, 1)
                piece = jnp.where(lane_8 // 32 == p, moved, piece)
            pieces.append(piece)
    parts = doubled(split_dot(halves(jnp.concatenate(pieces, axis=0)), halves(mw[...]), NT), lane_e)
    shares = [sides(lambda q: zrecv[v, q]) - one_dot(parts, cxb[:, v * cx:(v + 1) * cx]) for v in every]
    for v in every:
        out[v] = (field[v].reshape(rows, cx) - one_dot(pts[v], stack3(shares[v]))) * time_step

    for group in [x_halo, y_halo, z_halo, e_copies] + x_copies + y_copies + z_copies + stat_copies:
        for copy in group:
            copy.wait_send()


def finish(nv, solved, stats, update, norm, sem):
    copies = []
    for v in range(nv):
        copy = pltpu.make_async_copy(solved.at[v], update.at[v], sem.at[v])
        copy.start()
        copies.append(copy)
    for v in range(nv):
        norm[v] = stats[0, v]
    for copy in copies:
        copy.wait()


def shards(counts, flow_state, advection, inverse_x, inverse_y, inverse_z, reduced_x, reduced_y, reduced_z):
    nv, cz, cy, cx = flow_state.shape
    gx, gy, gz = counts
    rows = cz * cy
    cells = rows * cx * gx * gy * gz
    hbm = pl.BlockSpec(memory_space=pltpu.HBM)
    vmem = pl.BlockSpec(memory_space=pltpu.VMEM)
    dma = pltpu.SemaphoreType.DMA
    pack = -(-4 * nv // 8) * 8
    nc = 2 if gy == 2 else 4
    nd = max(8, gy * nc)
    nz = max(8, 2 * gz)
    width = 12 * cy
    group = cy * min(cz, max(1, 256 // cy))
    out, stats = pl.pallas_call(
        functools.partial(kernel, (counts, nv, cz, cy, cx, cells)),
        out_shape=(pltpu.VMEM((nv, rows, cx), f32), pltpu.VMEM((8, cx), f32)),
        in_specs=[hbm] * 8,
        out_specs=(vmem, vmem),
        scratch_shapes=[
            pltpu.VMEM((nv, (cz + 4) * cy, cx), f32),
            pltpu.VMEM((nv, (cy + 4) * cz, cx), f32),
            pltpu.VMEM((3, (cz + 4) * cy, cx), f32),
            pltpu.VMEM(((cz + 4) * cy, cx), f32),
            pltpu.VMEM((3, pack, rows), f32),
            pltpu.VMEM((nv, rows, cx), f32),
            pltpu.VMEM((nv, rows, cx), f32),
            pltpu.VMEM((nv, cz, cy, cx), f32),
            pltpu.VMEM((nv, rows, cx), f32),
            pltpu.VMEM((rows, cx), f32),
            pltpu.VMEM((nv, nd * cz, 12 * cz), bf16),
            pltpu.VMEM((nv, nz * cy, width), bf16),
            pltpu.VMEM((nv, rows, width), bf16),
            pltpu.VMEM((nv, rows, width), bf16),
            pltpu.VMEM((nv, 8 * cz, 8 * cz), bf16),
            pltpu.VMEM((nv, 8 * cz, 8 * cz), bf16),
            pltpu.VMEM((nv, group, group), bf16),
            pltpu.VMEM((nv, group, group), bf16),
            pltpu.VMEM((nv, 2 * cx, 2 * cx), bf16),
            pltpu.VMEM((nv, cy, nc * cx), f32),
            pltpu.VMEM((cx, gx * pack), f32),
            pltpu.VMEM((cx, gx * 32), f32),
            pltpu.VMEM((cx, nv * cx), f32),
            pltpu.VMEM((cx, nv * cx), bf16),
            pltpu.VMEM((gx, pack, rows), f32),
            pltpu.VMEM((nv, gy, nc * cz, cx), f32),
            pltpu.VMEM((nv, gy, nc * cz, cx), f32),
            pltpu.VMEM((nv, gz, 2 * cy, cx), f32),
            pltpu.VMEM((nv, gz, 2 * cy, cx), f32),
            pltpu.VMEM((gz, 8, cx), f32),
            pltpu.VMEM((gz * gx, 8, cx), f32),
            pltpu.VMEM((gz * gx, 1, cx), f32),
            pltpu.VMEM((gy, 1, cx), f32),
            pltpu.VMEM(inverse_x.shape, f32),
            pltpu.VMEM(inverse_y.shape, f32),
            pltpu.VMEM(inverse_z.shape, f32),
            pltpu.VMEM(reduced_x.shape, f32),
            pltpu.VMEM(reduced_y.shape, f32),
            pltpu.VMEM(reduced_z.shape, f32),
            pltpu.SMEM(advection.shape, f32),
            dma((nv,)),
            dma((7,)),
            dma((6,)), dma((6,)),
            dma((gx - 1,)), dma((gx - 1,)),
            dma((nv, gy - 1)), dma((nv, gy - 1)),
            dma((nv, gz - 1)), dma((nv, gz - 1)),
            dma((gz * gx,)), dma((gz * gx,)),
            dma((gz * gx,)), dma((gz * gx,)),
            dma((gy - 1,)), dma((gy - 1,)),
            pltpu.SemaphoreType.REGULAR,
        ],
        compiler_params=pltpu.CompilerParams(
            collective_id=0, has_side_effects=True, vmem_limit_bytes=60 * 1024 * 1024),
    )(flow_state.reshape(nv, rows, cx), advection, inverse_x, inverse_y, inverse_z, reduced_x, reduced_y, reduced_z)
    update, norm = pl.pallas_call(
        functools.partial(finish, nv),
        out_shape=(jax.ShapeDtypeStruct((nv, rows, cx), f32), jax.ShapeDtypeStruct((nv,), f32)),
        in_specs=[vmem, vmem],
        out_specs=(pl.BlockSpec(memory_space=pltpu.HBM), pl.BlockSpec(memory_space=pltpu.SMEM)),
        scratch_shapes=[dma((nv,))],
        compiler_params=pltpu.CompilerParams(vmem_limit_bytes=4 * 1024 * 1024),
    )(out, stats)
    return update.reshape(flow_state.shape), norm


def solution(mesh):
    counts = tuple(mesh.shape[axis] for axis in AXES)
    placed = (P(None, "gz", "gy", "gx"), P(), P(), P(), P(), P(), P(), P())
    return jax.shard_map(
        functools.partial(shards, counts),
        mesh=mesh,
        in_specs=placed,
        out_specs=(P(None, "gz", "gy", "gx"), P()),
        check_vma=False,
    )
```
